256 devices in a mesh: shard: 16 (over z, core), model: 4 (over y), unit: 4 (over x).
Axes of the slice: x: 4, y: 4, z: 8, core: 2. Of those that a mesh axis runs over, the one named last changes fastest.
Arguments:
- train_query: bfloat16 [16384, 4096], P(('unit', 'shard'), 'model'), parts along dimension 0, may hold values from -0.125 to 0.125
- low_query: bfloat16 [16384, 16], P(('unit', 'shard')), parts along dimension 0, may hold values from -0.09375 to 0.09375
- high_query: bfloat16 [64, 4096], P('unit', 'model'), parts along dimension 0, may hold values from -1.5 to 1.5
- train_key: bfloat16 [16384, 1024], P(('unit', 'shard'), 'model'), parts along dimension 0, may hold values from -0.125 to 0.125
- low_key: bfloat16 [16384, 16], P(('unit', 'shard')), parts along dimension 0, may hold values from -0.09375 to 0.09375
- high_key: bfloat16 [64, 1024], P('unit', 'model'), parts along dimension 0, may hold values from -1.5 to 1.5
- train_value: bfloat16 [16384, 1024], P(('unit', 'shard'), 'model'), parts along dimension 0, may hold values from -0.125 to 0.125
- low_value: bfloat16 [16384, 16], P(('unit', 'shard')), parts along dimension 0, may hold values from -0.09375 to 0.09375
- high_value: bfloat16 [64, 1024], P('unit', 'model'), parts along dimension 0, may hold values from -1.5 to 1.5
- norm_train: float32 [16384], P(('unit', 'shard', 'model')), parts along dimension 0, may hold values from 0.25 to 1.75
- norm_step: float32 [16384], P(('unit', 'shard', 'model')), parts along dimension 0, may hold values from -0.3 to 0.3
Outputs:
- serving_query: bfloat16 [16384, 4096], P('unit', 'model'), parts along dimension 0
- serving_key: bfloat16 [16384, 1024], P('unit', 'model'), parts along dimension 0
- serving_value: bfloat16 [16384, 1024], P('unit', 'model'), parts along dimension 0
- scale_query: float32 [16384], P(('unit', 'model')), parts along dimension 0
- scale_key: float32 [4096], P(('unit', 'model')), parts along dimension 0
- scale_value: float32 [4096], P(('unit', 'model')), parts along dimension 0
- serve_norm: bfloat16 [16384], P('unit'), parts along dimension 0
The draws below stay inside these ranges and needn't reach their ends.
There are 4 independent parts, one for each index of `unit`. The reference program is written for one: setup_inputs(seed, part) draws one part's arguments, and reference() takes and returns one part's arrays. A program takes and returns all parts, laid end to end along the dimension named above; each array names one. Nothing has to cross between parts.
All inputs are finite; a program needn't handle non-finite values. Where the reference program divides by a largest or mean magnitude, that divisor is 1e-20 or more.
Results may differ from the reference program's by a relative error of at most 0.001.
Values may be sent and summed in bfloat16 or wider, within the bound.
A program may use at most 64 MiB of HBM per device.

```python
import jax
import jax.numpy as jnp

D_MODEL = 4096
Q_DIM = 4096
KV_DIM = 1024
RANK = 16


def with_spikes(values, key, source, target, shards_of, factor):
    owner, partner = [(jnp.arange(values.shape[position]) // (values.shape[position] // shards_of)).reshape([-1 if axis == position else 1 for axis in range(values.ndim)]) for position in (source, target)]
    chosen = jax.random.permutation(key, shards_of)[partner]
    strong = (owner == chosen) | (owner == (partner + shards_of // 2) % shards_of)
    return jnp.where(strong, factor * values, values)


def block_levels(rng, extent, pieces, low, largest):
    loudness, own = 1.0, jax.random.fold_in(rng, 6)
    for dim, parts in pieces:
        steps = jnp.exp(jax.random.uniform(jax.random.fold_in(own, dim), (parts,), jnp.float32, low / len(pieces), largest / len(pieces)))
        loudness = loudness * jnp.repeat(steps, extent[dim] // parts).reshape([-1 if axis == dim else 1 for axis in range(len(extent))])
    return loudness


def bell_draw(key, dims, deviation, most, pieces=(), held_as=jnp.bfloat16):
    loudness = block_levels(key, dims, pieces, -0.22, 0.18) if pieces else 1.0
    drawn = jax.random.normal(key, dims, jnp.float32) * deviation * loudness
    return jnp.minimum(jnp.maximum(drawn, -most), most).astype(held_as)


def noise_with(rng, extent, width, most, shards, heavy, held_as=jnp.bfloat16):
    drawn = width * jax.random.normal(rng, extent, jnp.float32)
    if shards:
        drawn = drawn * block_levels(rng, extent, shards, -0.22, 0.18)
    return jnp.clip(with_spikes(drawn, jax.random.fold_in(rng, 3), *heavy), -most, most).astype(held_as)


def setup_inputs(seed: int = 0, part: int = 0) -> dict:
    key_list = jax.random.split(jax.random.key(seed), 12)
    part_splits = jax.random.split(jax.random.fold_in(key_list[11], part), 12)
    return {
        "train_query": noise_with(part_splits[0], (D_MODEL, Q_DIM), D_MODEL ** -0.5, 0.125, ((0, 16), (1, 4)), (0, 1, 16, 2.0)),
        "low_query": bell_draw(part_splits[1], (D_MODEL, RANK), D_MODEL ** -0.5, 0.09375, ((0, 16),)),
        "high_query": bell_draw(part_splits[2], (RANK, Q_DIM), RANK ** -0.5, 1.5, ((1, 4),)),
        "train_key": noise_with(part_splits[3], (D_MODEL, KV_DIM), D_MODEL ** -0.5, 0.125, ((0, 16), (1, 4)), (0, 1, 16, 2.0)),
        "low_key": bell_draw(part_splits[4], (D_MODEL, RANK), D_MODEL ** -0.5, 0.09375, ((0, 16),)),
        "high_key": bell_draw(part_splits[5], (RANK, KV_DIM), RANK ** -0.5, 1.5, ((1, 4),)),
        "train_value": noise_with(part_splits[6], (D_MODEL, KV_DIM), D_MODEL ** -0.5, 0.125, ((0, 16), (1, 4)), (0, 1, 16, 2.0)),
        "low_value": bell_draw(part_splits[7], (D_MODEL, RANK), D_MODEL ** -0.5, 0.09375, ((0, 16),)),
        "high_value": bell_draw(part_splits[8], (RANK, KV_DIM), RANK ** -0.5, 1.5, ((1, 4),)),
        "norm_train": jnp.clip(1.0 + 0.15 * jax.random.normal(part_splits[9], (D_MODEL,), jnp.float32), 0.25, 1.75),
        "norm_step": jnp.clip(jax.random.uniform(part_splits[10], (D_MODEL,), jnp.float32, -0.3, 0.3) * block_levels(part_splits[10], (D_MODEL,), ((0, 64),), -0.4, 0.0), -0.3, 0.3),
    }


mix_rate = 1.0


def reference(train_query, low_query, high_query, train_key, low_key, high_key, train_value, low_value, high_value, norm_train, norm_step):
    whole_query = train_query.astype(jnp.float32) + mix_rate * jnp.dot(low_query, high_query, preferred_element_type=jnp.float32)
    whole_key = train_key.astype(jnp.float32) + mix_rate * jnp.dot(low_key, high_key, preferred_element_type=jnp.float32)
    whole_value = train_value.astype(jnp.float32) + mix_rate * jnp.dot(low_value, high_value, preferred_element_type=jnp.float32)
    scale_query = jnp.max(jnp.abs(whole_query), axis=0)
    serving_query = (whole_query / scale_query).astype(jnp.bfloat16)
    scale_key = jnp.max(jnp.abs(whole_key), axis=0)
    serving_key = (whole_key / scale_key).astype(jnp.bfloat16)
    scale_value = jnp.max(jnp.abs(whole_value), axis=0)
    serving_value = (whole_value / scale_value).astype(jnp.bfloat16)
    serve_norm = (norm_train + norm_step).astype(jnp.bfloat16)
    return serving_query, serving_key, serving_value, scale_query, scale_key, scale_value, serve_norm
```

```python
import functools

import jax
import jax.numpy as jnp
from jax import lax
from jax.experimental import pallas as pl
from jax.experimental.pallas import tpu as pltpu
from jax.sharding import PartitionSpec as P

MESH = pl.DeviceIdType.MESH
F32, BF16 = jnp.float32, jnp.bfloat16
STEPS = 4
LOW, NORM = STEPS, STEPS + 1


def gather_kernel(
    count, models,
    q, k, v, low_q, low_k, low_v, high_q, high_k, high_v, norm_a, norm_b,
    whole, most, norms,
    raw, low_t, low_n, high, norm_in, norm_all, peak,
    in_sem, y_send, y_recv, ring_send, ring_recv, pair_send, pair_recv,
):
    me, my = lax.axis_index("shard"), lax.axis_index("model")
    right, left = lax.rem(me + 2, count), lax.rem(me + count - 2, count)
    partner = me + 1 - 2 * lax.rem(me, 2)
    over = partner - me
    rank = low_q.shape[0]
    half = raw.shape[1] // 2
    rows = half // STEPS
    hops = count // 4
    units = 2 * hops - 1
    widths = (q.shape[1], k.shape[1], v.shape[1])
    starts = (0, widths[0], widths[0] + widths[1])
    width = sum(widths)

    fetch = []
    for n, (src, start, wide) in enumerate(zip((q, k, v), starts, widths)):
        fetch.append(pltpu.make_async_copy(src, raw.at[me, :, pl.ds(start, wide)], in_sem.at[n]))
    for n, src in enumerate((low_q, low_k, low_v)):
        for h in range(2):
            fetch.append(
                pltpu.make_async_copy(
                    src.at[:, pl.ds(h * half, half)],
                    low_t.at[me, h, pl.ds(n * rank, rank)],
                    in_sem.at[3 + 2 * n + h],
                )
            )
    for n, (src, start, wide) in enumerate(zip((high_q, high_k, high_v), starts, widths)):
        fetch.append(
            pltpu.make_async_copy(src, high.at[pl.ds(n * rank, rank), pl.ds(start, wide)], in_sem.at[9 + n])
        )
    for n, src in enumerate((norm_a, norm_b)):
        fetch.append(pltpu.make_async_copy(src, norm_in.at[n], in_sem.at[12 + n]))
    for copy in fetch:
        copy.start()

    barrier = pltpu.get_barrier_semaphore()
    for other in (partner, right, left):
        pl.semaphore_signal(barrier, inc=1, device_id={"shard": other}, device_id_type=MESH)
    for step in range(1, models):
        pl.semaphore_signal(
            barrier, inc=1, device_id={"model": lax.rem(my + step, models)}, device_id_type=MESH
        )
    for n in range(3):
        for m in range(3):
            if n != m:
                high[n * rank : (n + 1) * rank, starts[m] : starts[m] + widths[m]] = jnp.zeros(
                    (rank, widths[m]), BF16
                )
    peak[...] = jnp.zeros_like(peak)
    pl.semaphore_wait(barrier, 3 + models - 1)

    def part(p, h, j):
        if isinstance(j, int) and j == LOW:
            return low_t.at[p, h]
        if isinstance(j, int) and j == NORM:
            return norm_all.at[p, pl.ds(h * (models // 2), models // 2)]
        return raw.at[p, pl.ds(pl.multiple_of(h * half + j * rows, rows), rows)]

    def hop(way, u, j, p, h):
        ref = part(p, h, j)
        return pltpu.make_async_remote_copy(
            src_ref=ref, dst_ref=ref,
            send_sem=ring_send.at[way, u, j], recv_sem=ring_recv.at[way, u, j],
            device_id={"shard": (right, left)[way]}, device_id_type=MESH,
        )

    def hand(way, u, j, p, h):
        ref = part(p, h, j)
        return pltpu.make_async_remote_copy(
            src_ref=ref, dst_ref=ref,
            send_sem=pair_send.at[way, u, j], recv_sem=pair_recv.at[way, u, j],
            device_id={"shard": partner}, device_id_type=MESH,
        )

    def halves(way, u):
        h = lax.rem(u, 2)
        return h if way == 0 else 1 - h

    def origin(way, u):
        far = 2 * (u // 2 + 1)
        return lax.rem(me + count - far, count) if way == 0 else lax.rem(me + far, count)

    for copy in fetch[:3]:
        copy.wait()

    def send_own(n, j):
        for way in range(2):
            hop(way, n, j, me, n if way == 0 else 1 - n).start()
        hand(2, n, j, me, n).start()

    send_own(0, 0)
    for copy in fetch[3:]:
        copy.wait()
    norm_all[me, my] = norm_in[0] + norm_in[1]
    for j in range(1, STEPS):
        send_own(0, j)
    send_own(0, LOW)
    across = []
    for step in range(1, models):
        ref = norm_all.at[me, my]
        copy = pltpu.make_async_remote_copy(
            src_ref=ref, dst_ref=ref, send_sem=y_send.at[step], recv_sem=y_recv.at[step],
            device_id={"model": lax.rem(my + step, models)}, device_id_type=MESH,
        )
        copy.start()
        across.append(copy)
    for j in range(STEPS):
        send_own(1, j)
    send_own(1, LOW)

    def unfold(slot, p, h):
        low_n[slot] = jnp.transpose(low_t[p, h].astype(F32), (1, 0)).astype(BF16)

    def merge(slot, p, h, s):
        at = pl.ds(pl.multiple_of(h * half + s * rows, rows), rows)
        low = low_n[slot, pl.ds(pl.multiple_of(s * rows, rows), rows), :]
        block = 512
        for c in range(0, width, block):
            cols = slice(c, c + block)
            new = raw[p, at, cols].astype(F32) + jnp.dot(low, high[:, cols], preferred_element_type=F32)
            whole[p, at, cols] = new
            peak[:, cols] = jnp.maximum(
                peak[:, cols], jnp.max(jnp.abs(new).reshape(rows // 8, 8, block), axis=0)
            )

    def merge_half(p, h):
        unfold(0, p, h)

        @pl.loop(0, STEPS)
        def _(s):
            merge(0, p, h, s)

    for h in range(2):
        merge_half(me, h)
    for step in range(1, models):
        across[step - 1].wait_recv()
    for n in range(2):
        send_own(n, NORM)
    for h in range(2):
        for j in range(STEPS + 2):
            hand(2, h, j, partner, h).wait_recv()
        merge_half(partner, h)

    def from_ring(way, u, j, p, h):
        hop(way, u, j, p, h).wait_recv()

        @pl.when(u < units - 2)
        def _():
            hop(way, u + 2, j, p, h).start()

        hand(way, u, j, p, h).start()

    def from_pair(e):
        u, s = e // STEPS, lax.rem(e, STEPS)
        for way in range(2):
            p, h = origin(way, u) + over, halves(way, u)
            hand(way, u, s, p, h).wait_recv()

            @pl.when(s == 0)
            def _():
                hand(way, u, LOW, p, h).wait_recv()
                unfold(2 + way, p, h)

            @pl.when(s == STEPS - 1)
            def _():
                hand(way, u, NORM, p, h).wait_recv()

            merge(2 + way, p, h, s)

    @pl.loop(0, units * STEPS)
    def _(e):
        u, s = e // STEPS, lax.rem(e, STEPS)
        for way in range(2):
            p, h = origin(way, u), halves(way, u)
            from_ring(way, u, s, p, h)

            @pl.when(s == 0)
            def _():
                from_ring(way, u, LOW, p, h)
                unfold(way, p, h)

            @pl.when(s == STEPS - 1)
            def _():
                from_ring(way, u, NORM, p, h)

        for way in range(2):
            merge(way, origin(way, u), halves(way, u), s)

        @pl.when(e > 0)
        def _():
            from_pair(e - 1)

    from_pair(units * STEPS - 1)

    most[...] = peak[...]
    norms[...] = norm_all[...]

    @pl.loop(0, units)
    def _(u):
        for j in range(STEPS + 2):
            for way in range(2):
                hop(way, u, j, me, 0).wait_send()
                hand(way, u, j, me, 0).wait_send()

    for n in range(2):
        for j in range(STEPS + 2):
            hand(2, n, j, me, n).wait_send()
    for copy in across:
        copy.wait_send()


def serve_kernel(
    whole, most, norms,
    q, k, v, scale_q, scale_k, scale_v, norm,
    q_out, k_out, v_out, scale_out, norm_f, norm_out,
    big_sem, sem,
):
    pieces, deep, width = whole.shape
    outs, stages = (q, k, v), (q_out, k_out, v_out)
    widths = tuple(a.shape[1] for a in outs)
    starts = (0, widths[0], widths[0] + widths[1])
    scale_out[...] = jnp.max(most[...], axis=0, keepdims=True)
    small = []
    for n, (dst, start, wide) in enumerate(zip((scale_q, scale_k, scale_v), starts, widths)):
        small.append(pltpu.make_async_copy(scale_out.at[:, pl.ds(start, wide)], dst, sem.at[n]))
    rows = 32

    def out(n, p):
        at = pl.ds(pl.multiple_of(p * deep, deep), deep)
        return pltpu.make_async_copy(stages[n].at[at], outs[n].at[at], big_sem.at[n, p])

    @pl.loop(0, pieces)
    def _(p):
        @pl.loop(0, deep // rows)
        def _(r):
            here = pl.ds(pl.multiple_of(r * rows, rows), rows)
            there = pl.ds(pl.multiple_of(p * deep + r * rows, rows), rows)
            for n in range(3):
                cols = slice(starts[n], starts[n] + widths[n])
                stages[n][there, :] = (whole[p, here, cols] * (1.0 / scale_out[:, cols])).astype(BF16)

        for n in range(3):
            out(n, p).start()

    models = norms.shape[1]
    wide = norms.shape[3]
    for m in range(0, models, 2):
        pair = jnp.concatenate([norms[:, m, 0, :], norms[:, m + 1, 0, :]], axis=1)
        norm_f[pl.ds(m // 2, pieces, stride=models // 2), :] = pair
    norm_out[...] = norm_f[...].astype(BF16)
    small.append(pltpu.make_async_copy(norm_out, norm, sem.at[3]))
    for copy in small:
        copy.start()
    for copy in small:
        copy.wait()

    @pl.loop(0, pieces)
    def _(p):
        for n in range(3):
            out(n, p).wait()


def local(count, models, q, low_q, high_q, k, low_k, high_k, v, low_v, high_v, norm_train, norm_step):
    deep, rank = low_q.shape
    widths = (q.shape[1], k.shape[1], v.shape[1])
    width = sum(widths)
    units = count // 2 - 1
    piece = norm_train.shape[0]
    dma = pltpu.SemaphoreType.DMA
    anywhere = pl.BlockSpec(memory_space=pl.ANY)
    vmem = pl.BlockSpec(memory_space=pltpu.VMEM)
    whole, most, norms = pl.pallas_call(
        functools.partial(gather_kernel, count, models),
        out_shape=(
            pltpu.VMEM((count, deep, width), F32),
            pltpu.VMEM((8, width), F32),
            pltpu.VMEM((count, models, 1, piece), F32),
        ),
        in_specs=[anywhere] * 11,
        out_specs=(vmem, vmem, vmem),
        scratch_shapes=[
            pltpu.VMEM((count, deep, width), BF16),
            pltpu.VMEM((count, 2, 3 * rank, deep // 2), BF16),
            pltpu.VMEM((4, deep // 2, 3 * rank), BF16),
            pltpu.VMEM((3 * rank, width), BF16),
            pltpu.VMEM((2, 1, piece), F32),
            pltpu.VMEM((count, models, 1, piece), F32),
            pltpu.VMEM((8, width), F32),
            dma((14,)),
            dma((models,)),
            dma((models,)),
            dma((2, units, STEPS + 2)),
            dma((2, units, STEPS + 2)),
            dma((3, units, STEPS + 2)),
            dma((3, units, STEPS + 2)),
        ],
        compiler_params=pltpu.CompilerParams(
            collective_id=0, has_side_effects=True, vmem_limit_bytes=20 * 2**20
        ),
        name="gather",
    )(
        *(
            pltpu.with_memory_space_constraint(a, pltpu.HBM)
            for a in (
                q, k, v, low_q.T, low_k.T, low_v.T, high_q, high_k, high_v,
                norm_train.reshape(1, piece), norm_step.reshape(1, piece),
            )
        )
    )
    total = count * deep
    sizes = tuple((total, w) for w in widths)
    serving_q, serving_k, serving_v, scale_q, scale_k, scale_v, norm = pl.pallas_call(
        serve_kernel,
        out_shape=tuple(jax.ShapeDtypeStruct(s, BF16) for s in sizes)
        + tuple(jax.ShapeDtypeStruct((1, w), F32) for w in widths)
        + (jax.ShapeDtypeStruct((count * models // 2, 2 * piece), BF16),),
        in_specs=[vmem] * 3,
        out_specs=(anywhere,) * 7,
        scratch_shapes=[pltpu.VMEM(s, BF16) for s in sizes]
        + [
            pltpu.VMEM((1, width), F32),
            pltpu.VMEM((count * models // 2, 2 * piece), F32),
            pltpu.VMEM((count * models // 2, 2 * piece), BF16),
            dma((3, count)),
            dma((4,)),
        ],
        compiler_params=pltpu.CompilerParams(vmem_limit_bytes=20 * 2**20),
        name="serve",
    )(*(pltpu.with_memory_space_constraint(a, pltpu.VMEM) for a in (whole, most, norms)))
    return (
        serving_q, serving_k, serving_v,
        scale_q.reshape(-1), scale_k.reshape(-1), scale_v.reshape(-1), norm.reshape(-1),
    )


def solution(mesh):
    in_specs = (
        P(("unit", "shard"), "model"),
        P(("unit", "shard"), None),
        P("unit", "model"),
        P(("unit", "shard"), "model"),
        P(("unit", "shard"), None),
        P("unit", "model"),
        P(("unit", "shard"), "model"),
        P(("unit", "shard"), None),
        P("unit", "model"),
        P(("unit", "shard", "model")),
        P(("unit", "shard", "model")),
    )
    out_specs = (
        P("unit", "model"),
        P("unit", "model"),
        P("unit", "model"),
        P(("unit", "model")),
        P(("unit", "model")),
        P(("unit", "model")),
        P("unit"),
    )
    body = functools.partial(local, mesh.shape["shard"], mesh.shape["model"])
    return jax.shard_map(body, mesh=mesh, in_specs=in_specs, out_specs=out_specs, check_vma=False)
```

```python
import functools

import jax
import jax.numpy as jnp
from jax import lax
from jax.experimental import pallas as pl
from jax.experimental.pallas import tpu as pltpu
from jax.sharding import PartitionSpec as P

MESH = pl.DeviceIdType.MESH
F32, BF16 = jnp.float32, jnp.bfloat16
ROWS = ((0, 64), (64, 32), (96, 16), (112, 16))


def gather_kernel(
    count, models,
    q, k, v, low_q, low_k, low_v, high_q, high_k, high_v, norm_a, norm_b,
    whole, most, norms,
    raw, extra, low_n, high, norm_in, peak,
    in_sem, y_send, y_recv, ring_send, ring_recv, pair_send, pair_recv,
):
    me, my = lax.axis_index("shard"), lax.axis_index("model")
    right, left = lax.rem(me + 2, count), lax.rem(me + count - 2, count)
    partner = me + 1 - 2 * lax.rem(me, 2)
    over = partner - me
    rank = low_q.shape[0]
    half = raw.shape[1] // 2
    hops = count // 4
    full = 2 * (hops - 1)
    widths = (q.shape[1], k.shape[1], v.shape[1])
    starts = (0, widths[0], widths[0] + widths[1])
    width = sum(widths)

    fetch = []
    for n, (src, start, wide) in enumerate(zip((q, k, v), starts, widths)):
        fetch.append(pltpu.make_async_copy(src, raw.at[me, :, pl.ds(start, wide)], in_sem.at[n]))
    at = (
        pl.ds(pl.multiple_of(lax.div(my, 2) * 8, 8), 8),
        pl.ds(pl.multiple_of(lax.rem(my, 2) * half, half), half),
    )
    for n, src in enumerate((low_q, low_k, low_v)):
        fetch.append(pltpu.make_async_copy(src.at[at], extra.at[me, my, n], in_sem.at[3 + n]))
    for n, (src, start, wide) in enumerate(zip((high_q, high_k, high_v), starts, widths)):
        fetch.append(
            pltpu.make_async_copy(src, high.at[pl.ds(n * rank, rank), pl.ds(start, wide)], in_sem.at[6 + n])
        )
    for n, src in enumerate((norm_a, norm_b)):
        fetch.append(pltpu.make_async_copy(src, norm_in.at[n], in_sem.at[9 + n]))
    for copy in fetch[9:] + fetch[:9]:
        copy.start()

    barrier = pltpu.get_barrier_semaphore()
    for other in (partner, right, left):
        pl.semaphore_signal(barrier, inc=1, device_id={"shard": other}, device_id_type=MESH)
    for step in range(1, models):
        pl.semaphore_signal(
            barrier, inc=1, device_id={"model": lax.rem(my + step, models)}, device_id_type=MESH
        )
    for copy in fetch[9:]:
        copy.wait()
    total = norm_in[0] + norm_in[1]
    spread = jnp.concatenate([total, jnp.zeros((1, 128 - total.shape[1]), F32)], axis=1)
    extra[me, my, 3] = jnp.broadcast_to(spread, (8, 128)).astype(BF16)
    for n in range(3):
        for m in range(3):
            if n != m:
                high[n * rank : (n + 1) * rank, starts[m] : starts[m] + widths[m]] = jnp.zeros(
                    (rank, widths[m]), BF16
                )
    peak[...] = jnp.zeros_like(peak)
    for copy in fetch[:9]:
        copy.wait()
    pl.semaphore_wait(barrier, 3 + models - 1)

    def block(p):
        return extra.at[p, my]

    def span(p, h, first=0, rows=half):
        return raw.at[p, pl.ds(pl.multiple_of(h * half + first, 16), rows)]

    def send(ref, sends, recvs, index, to):
        return pltpu.make_async_remote_copy(
            src_ref=ref, dst_ref=ref, send_sem=sends.at[index], recv_sem=recvs.at[index],
            device_id=to, device_id_type=MESH,
        )

    def hop(way, j, ref):
        return send(ref, ring_send, ring_recv, (way, j), {"shard": (right, left)[way]})

    def hand(way, j, ref):
        return send(ref, pair_send, pair_recv, (way, j), {"shard": partner})

    def across(slot, p):
        return [
            send(block(p), y_send, y_recv, (slot, step - 1), {"model": lax.rem(my + step, models)})
            for step in range(1, models)
        ]

    def origin(way, hop_count):
        far = 2 * (hop_count + 1)
        return lax.rem(me + count + (2 * way - 1) * far, count)

    def slot_of(way, kk):
        return 2 + 2 * kk + 2 * hops * way

    def half_of(way, u):
        return lax.rem(u + way, 2)

    HALF, LAST = hops, hops + full

    for way in range(2):
        hop(way, 0, block(me)).start()
        hop(way, HALF, span(me, way)).start()
    hand(2, 0, block(me)).start()
    for copy in across(0, me):
        copy.start()
    hand(2, 1, raw.at[me]).start()
    for way in range(2):
        hop(way, HALF + 1, span(me, 1 - way)).start()

    def unfold(slot, p, h):
        parts = [
            extra[p, quarter + h, n].astype(F32)
            for n in range(3)
            for quarter in range(0, models, 2)
        ]
        low_n[slot] = jnp.transpose(jnp.concatenate(parts, axis=0), (1, 0)).astype(BF16)

    def merge(slot, p, h, first, rows):
        low = low_n[slot, pl.ds(pl.multiple_of(first, 16), rows), :]
        at = pl.ds(pl.multiple_of(h * half + first, 16), rows)
        wide = 512
        for c in range(0, width, wide):
            cols = slice(c, c + wide)
            new = raw[p, at, cols].astype(F32) + jnp.dot(low, high[:, cols], preferred_element_type=F32)
            whole[p, at, cols] = new
            peak[:, cols] = jnp.maximum(
                peak[:, cols], jnp.max(jnp.abs(new).reshape(rows // 8, 8, wide), axis=0)
            )

    def merge_four(which):
        @pl.loop(0, 4)
        def _(j):
            p, h = which(lax.div(j, 2), lax.rem(j, 2))
            unfold(0, p, h)

            @pl.loop(0, half // 32)
            def _(s):
                merge(0, p, h, s * 32, 32)

    def wait_across(slots):
        for slot in slots:
            for copy in across(slot, me):
                copy.wait_recv()

    def merge_event(event):
        if event == 0:
            wait_across((0, 1))
            hand(2, 1, raw.at[partner]).wait_recv()
            merge_four(lambda way, other: (me + other * over, way))
            return
        u = event - 1
        kk = u // 2
        if u % 2 == 0:
            wait_across([slot_of(way, kk) + other for way in range(2) for other in range(2)])
        merge_four(lambda way, other: (origin(way, kk) + other * over, half_of(way, u)))

    def ways(kk):
        return range(2 if kk < hops - 1 else 1)

    def from_pair(event):
        if event == 0:
            hand(2, 0, block(partner)).wait_recv()
            for copy in across(1, partner):
                copy.start()
            return
        u = event - 1
        if event <= hops:
            for way in ways(event - 1):
                p = origin(way, event - 1) + over
                hand(way, event - 1, block(p)).wait_recv()
                for copy in across(slot_of(way, event - 1) + 1, p):
                    copy.start()
        for way in range(2):
            hand(way, HALF + u, span(origin(way, u // 2) + over, half_of(way, u))).wait_recv()

    done = 0
    for event in range(1, full + 1):
        u = event - 1
        kk = u // 2
        for way in range(2):
            p, h = origin(way, kk), half_of(way, u)
            hop(way, HALF + u, span(p, h)).wait_recv()
            if event <= hops and way in ways(event - 1):
                e = origin(way, event - 1)
                hop(way, event - 1, block(e)).wait_recv()
                if way in ways(event) and event < hops:
                    hop(way, event, block(e)).start()
                hand(way, event - 1, block(e)).start()
                for copy in across(slot_of(way, event - 1), e):
                    copy.start()
            if u + 2 < full:
                hop(way, HALF + u + 2, span(p, h)).start()
            elif u + 2 == full:
                for j, (first, rows) in enumerate(ROWS):
                    hop(way, LAST + j, span(p, h, first, rows)).start()
            hand(way, HALF + u, span(p, h)).start()
        from_pair(event - 1)
        if event >= 2:
            merge_event(event - 2)
            done = event - 2
    from_pair(full)
    for event in range(done + 1, full + 1):
        merge_event(event)

    wait_across([slot_of(0, hops - 1) + other for other in range(2)])
    far = origin(0, hops - 1)
    for way in range(2):
        for other in range(2):
            unfold(2 * way + other, far + other * over, way)

    @pl.loop(0, count)
    def _(p):
        norms[p] = extra[p, :, 3]

    def sent(copies):
        for copy in copies:
            copy.wait_send()

    for slot in range(4 * hops):
        sent(across(slot, me))
    sent([hand(2, 0, block(me)), hand(2, 1, raw.at[me])])
    for way in range(2):
        for kk in range(hops):
            if way in ways(kk):
                sent([hop(way, kk, block(me)), hand(way, kk, block(me))])
        for u in range(full):
            sent([hand(way, HALF + u, span(me, 0))])
        for u in range(full - 2):
            sent([hop(way, HALF + u, span(me, 0))])

    def last_pair(j):
        first, rows = ROWS[j]
        for way in range(2):
            hand(way, LAST + j, span(far + over, way, first, rows)).wait_recv()
            merge(2 * way + 1, far + over, way, first, rows)

    for j, (first, rows) in enumerate(ROWS):
        for way in range(2):
            hop(way, LAST + j, span(far, way, first, rows)).wait_recv()
            hand(way, LAST + j, span(far, way, first, rows)).start()
        if j > 0:
            last_pair(j - 1)
        for way in range(2):
            merge(2 * way, far, way, first, rows)
    last_pair(len(ROWS) - 1)
    most[...] = peak[...]

    for way in range(2):
        for u in range(full - 2, full):
            sent([hop(way, HALF + u, span(me, 0))])
        for j, (first, rows) in enumerate(ROWS):
            sent([hop(way, LAST + j, span(me, 0, first, rows)), hand(way, LAST + j, span(me, 0, first, rows))])


def serve_kernel(
    whole, most, norms,
    q, k, v, scale_q, scale_k, scale_v, norm,
    q_out, k_out, v_out, scale_out, per, norm_f, norm_out,
    big_sem, sem,
):
    pieces, deep, width = whole.shape
    outs, stages = (q, k, v), (q_out, k_out, v_out)
    widths = tuple(a.shape[1] for a in outs)
    starts = (0, widths[0], widths[0] + widths[1])
    scale_out[...] = jnp.max(most[...], axis=0, keepdims=True)
    small = []
    for n, (dst, start, wide) in enumerate(zip((scale_q, scale_k, scale_v), starts, widths)):
        small.append(pltpu.make_async_copy(scale_out.at[:, pl.ds(start, wide)], dst, sem.at[n]))
    per[...] = 1.0 / scale_out[...]
    rows = 32

    def out(n, p):
        at = pl.ds(pl.multiple_of(p * deep, deep), deep)
        return pltpu.make_async_copy(stages[n].at[at], outs[n].at[at], big_sem.at[n, p])

    @pl.loop(0, pieces)
    def _(p):
        @pl.loop(0, deep // rows)
        def _(r):
            here = pl.ds(pl.multiple_of(r * rows, rows), rows)
            there = pl.ds(pl.multiple_of(p * deep + r * rows, rows), rows)
            for n in range(3):
                cols = slice(starts[n], starts[n] + widths[n])
                stages[n][there, :] = (whole[p, here, cols] * per[:, cols]).astype(BF16)

        for n in range(3):
            out(n, p).start()

    models = norms.shape[1]
    wide = norm_f.shape[1] // 2
    for m in range(0, models, 2):
        pair = jnp.concatenate(
            [norms[:, n].astype(F32)[:, 0, :wide] for n in (m, m + 1)], axis=1
        )
        norm_f[pl.ds(m // 2, pieces, stride=models // 2), :] = pair
    norm_out[...] = norm_f[...].astype(BF16)
    small.append(pltpu.make_async_copy(norm_out, norm, sem.at[3]))
    for copy in small:
        copy.start()
    for copy in small:
        copy.wait()

    @pl.loop(0, pieces)
    def _(p):
        for n in range(3):
            out(n, p).wait()


def local(count, models, q, low_q, high_q, k, low_k, high_k, v, low_v, high_v, norm_train, norm_step):
    deep, rank = low_q.shape
    widths = (q.shape[1], k.shape[1], v.shape[1])
    width = sum(widths)
    copies = count // 4 + 2 * (count // 4 - 1) + len(ROWS)
    piece = norm_train.shape[0]
    dma = pltpu.SemaphoreType.DMA
    anywhere = pl.BlockSpec(memory_space=pl.ANY)
    vmem = pl.BlockSpec(memory_space=pltpu.VMEM)
    whole, most, norms = pl.pallas_call(
        functools.partial(gather_kernel, count, models),
        out_shape=(
            pltpu.VMEM((count, deep, width), F32),
            pltpu.VMEM((8, width), F32),
            pltpu.VMEM((count, models, 8, 128), BF16),
        ),
        in_specs=[anywhere] * 11,
        out_specs=(vmem, vmem, vmem),
        scratch_shapes=[
            pltpu.VMEM((count, deep, width), BF16),
            pltpu.VMEM((count, models, 4, 8, 128), BF16),
            pltpu.VMEM((4, deep // 2, 3 * rank), BF16),
            pltpu.VMEM((3 * rank, width), BF16),
            pltpu.VMEM((2, 1, piece), F32),
            pltpu.VMEM((8, width), F32),
            dma((11,)),
            dma((count, models - 1)),
            dma((count, models - 1)),
            dma((2, copies)),
            dma((2, copies)),
            dma((3, copies)),
            dma((3, copies)),
        ],
        compiler_params=pltpu.CompilerParams(
            collective_id=0, has_side_effects=True, vmem_limit_bytes=20 * 2**20
        ),
        name="gather",
    )(
        *(
            pltpu.with_memory_space_constraint(a, pltpu.HBM)
            for a in (
                q, k, v, low_q.T, low_k.T, low_v.T, high_q, high_k, high_v,
                norm_train.reshape(1, piece), norm_step.reshape(1, piece),
            )
        )
    )
    total = count * deep
    sizes = tuple((total, w) for w in widths)
    serving_q, serving_k, serving_v, scale_q, scale_k, scale_v, norm = pl.pallas_call(
        serve_kernel,
        out_shape=tuple(jax.ShapeDtypeStruct(s, BF16) for s in sizes)
        + tuple(jax.ShapeDtypeStruct((1, w), F32) for w in widths)
        + (jax.ShapeDtypeStruct((count * models // 2, 2 * piece), BF16),),
        in_specs=[vmem] * 3,
        out_specs=(anywhere,) * 7,
        scratch_shapes=[pltpu.VMEM(s, BF16) for s in sizes]
        + [
            pltpu.VMEM((1, width), F32),
            pltpu.VMEM((1, width), F32),
            pltpu.VMEM((count * models // 2, 2 * piece), F32),
            pltpu.VMEM((count * models // 2, 2 * piece), BF16),
            dma((3, count)),
            dma((4,)),
        ],
        compiler_params=pltpu.CompilerParams(vmem_limit_bytes=20 * 2**20),
        name="serve",
    )(*(pltpu.with_memory_space_constraint(a, pltpu.VMEM) for a in (whole, most, norms)))
    return (
        serving_q, serving_k, serving_v,
        scale_q.reshape(-1), scale_k.reshape(-1), scale_v.reshape(-1), norm.reshape(-1),
    )


def solution(mesh):
    in_specs = (
        P(("unit", "shard"), "model"),
        P(("unit", "shard"), None),
        P("unit", "model"),
        P(("unit", "shard"), "model"),
        P(("unit", "shard"), None),
        P("unit", "model"),
        P(("unit", "shard"), "model"),
        P(("unit", "shard"), None),
        P("unit", "model"),
        P(("unit", "shard", "model")),
        P(("unit", "shard", "model")),
    )
    out_specs = (
        P("unit", "model"),
        P("unit", "model"),
        P("unit", "model"),
        P(("unit", "model")),
        P(("unit", "model")),
        P(("unit", "model")),
        P("unit"),
    )
    body = functools.partial(local, mesh.shape["shard"], mesh.shape["model"])
    return jax.shard_map(body, mesh=mesh, in_specs=in_specs, out_specs=out_specs, check_vma=False)
```

```python
import functools

import jax
import jax.numpy as jnp
from jax import lax
from jax.experimental import pallas as pl
from jax.experimental.pallas import tpu as pltpu
from jax.sharding import PartitionSpec as P

MESH = pl.DeviceIdType.MESH
F32, BF16 = jnp.float32, jnp.bfloat16
ROWS = ((0, 64), (64, 32), (96, 16), (112, 16))


def gather_kernel(
    count, models,
    q, k, v, low_q, low_k, low_v, high_q, high_k, high_v, norm_a, norm_b,
    whole, most, norms,
    raw, extra, low_n, high, norm_in, peak,
    in_sem, y_send, y_recv, ring_send, ring_recv, pair_send, pair_recv,
):
    me, my = lax.axis_index("shard"), lax.axis_index("model")
    right, left = lax.rem(me + 2, count), lax.rem(me + count - 2, count)
    partner = me + 1 - 2 * lax.rem(me, 2)
    over = partner - me
    rank = low_q.shape[0]
    half = raw.shape[1] // 2
    hops = count // 4
    full = 2 * (hops - 1)
    widths = (q.shape[1], k.shape[1], v.shape[1])
    starts = (0, widths[0], widths[0] + widths[1])
    width = sum(widths)

    fetch = []
    for n, (src, start, wide) in enumerate(zip((q, k, v), starts, widths)):
        fetch.append(pltpu.make_async_copy(src, raw.at[me, :, pl.ds(start, wide)], in_sem.at[n]))
    at = (
        pl.ds(pl.multiple_of(lax.div(my, 2) * 8, 8), 8),
        pl.ds(pl.multiple_of(lax.rem(my, 2) * half, half), half),
    )
    for n, src in enumerate((low_q, low_k, low_v)):
        fetch.append(pltpu.make_async_copy(src.at[at], extra.at[me, my, n], in_sem.at[3 + n]))
    for n, (src, start, wide) in enumerate(zip((high_q, high_k, high_v), starts, widths)):
        fetch.append(
            pltpu.make_async_copy(src, high.at[pl.ds(n * rank, rank), pl.ds(start, wide)], in_sem.at[6 + n])
        )
    for n, src in enumerate((norm_a, norm_b)):
        fetch.append(pltpu.make_async_copy(src, norm_in.at[n], in_sem.at[9 + n]))
    for copy in fetch[9:] + fetch[:9]:
        copy.start()

    barrier = pltpu.get_barrier_semaphore()
    for other in (partner, right, left):
        pl.semaphore_signal(barrier, inc=1, device_id={"shard": other}, device_id_type=MESH)
    for step in range(1, models):
        pl.semaphore_signal(
            barrier, inc=1, device_id={"model": lax.rem(my + step, models)}, device_id_type=MESH
        )
    for copy in fetch[9:]:
        copy.wait()
    total = norm_in[0] + norm_in[1]
    spread = jnp.concatenate([total, jnp.zeros((1, 128 - total.shape[1]), F32)], axis=1)
    extra[me, my, 3] = jnp.broadcast_to(spread, (8, 128)).astype(BF16)
    for n in range(3):
        for m in range(3):
            if n != m:
                high[n * rank : (n + 1) * rank, starts[m] : starts[m] + widths[m]] = jnp.zeros(
                    (rank, widths[m]), BF16
                )
    peak[...] = jnp.zeros_like(peak)
    for copy in fetch[:9]:
        copy.wait()
    pl.semaphore_wait(barrier, 3 + models - 1)

    def block(p):
        return extra.at[p, my]

    def span(p, h, first=0, rows=half):
        return raw.at[p, pl.ds(pl.multiple_of(h * half + first, 16), rows)]

    def send(ref, sends, recvs, index, to):
        return pltpu.make_async_remote_copy(
            src_ref=ref, dst_ref=ref, send_sem=sends.at[index], recv_sem=recvs.at[index],
            device_id=to, device_id_type=MESH,
        )

    def hop(way, j, ref):
        return send(ref, ring_send, ring_recv, (way, j), {"shard": (right, left)[way]})

    def hand(way, j, ref):
        return send(ref, pair_send, pair_recv, (way, j), {"shard": partner})

    def across(slot, p):
        return [
            send(block(p), y_send, y_recv, (slot, step - 1), {"model": lax.rem(my + step, models)})
            for step in range(1, models)
        ]

    def origin(way, hop_count):
        far = 2 * (hop_count + 1)
        return lax.rem(me + count + (2 * way - 1) * far, count)

    def slot_of(way, kk):
        return 2 + 2 * kk + 2 * hops * way

    def half_of(way, u):
        return lax.rem(u + way, 2)

    HALF, LAST = hops, hops + full

    for way in range(2):
        hop(way, 0, block(me)).start()
        hop(way, HALF, span(me, way)).start()
    hand(2, 0, block(me)).start()
    for copy in across(0, me):
        copy.start()
    hand(2, 1, raw.at[me]).start()
    for way in range(2):
        hop(way, HALF + 1, span(me, 1 - way)).start()

    def unfold(slot, p, h):
        parts = [
            extra[p, quarter + h, n].astype(F32)
            for n in range(3)
            for quarter in range(0, models, 2)
        ]
        low_n[slot] = jnp.transpose(jnp.concatenate(parts, axis=0), (1, 0)).astype(BF16)

    def merge(slot, p, h, first, rows, ready=False):
        low = low_n[slot, pl.ds(pl.multiple_of(first, 16), rows), :]
        at = pl.ds(pl.multiple_of(h * half + first, 16), rows)
        wide = 256
        for c in range(0, width, wide):
            cols = slice(c, c + wide)
            add = (
                whole[p, at, cols]
                if ready
                else jnp.dot(low, high[:, cols], preferred_element_type=F32)
            )
            new = raw[p, at, cols].astype(F32) + add
            whole[p, at, cols] = new
            peak[:, cols] = jnp.maximum(
                peak[:, cols], jnp.max(jnp.abs(new).reshape(rows // 8, 8, wide), axis=0)
            )

    def merge_four(which):
        @pl.loop(0, 4)
        def _(j):
            p, h = which(lax.div(j, 2), lax.rem(j, 2))
            unfold(0, p, h)
            merge(0, p, h, 0, half)

    def wait_across(slots):
        for slot in slots:
            for copy in across(slot, me):
                copy.wait_recv()

    def merge_event(event):
        if event == 0:
            wait_across((0, 1))
            hand(2, 1, raw.at[partner]).wait_recv()
            merge_four(lambda way, other: (me + other * over, way))
            return
        u = event - 1
        kk = u // 2
        if u % 2 == 0:
            wait_across([slot_of(way, kk) + other for way in range(2) for other in range(2)])
        merge_four(lambda way, other: (origin(way, kk) + other * over, half_of(way, u)))

    def ways(kk):
        return range(2 if kk < hops - 1 else 1)

    def from_pair(event):
        if event == 0:
            hand(2, 0, block(partner)).wait_recv()
            for copy in across(1, partner):
                copy.start()
            return
        u = event - 1
        if event <= hops:
            for way in ways(event - 1):
                p = origin(way, event - 1) + over
                hand(way, event - 1, block(p)).wait_recv()
                for copy in across(slot_of(way, event - 1) + 1, p):
                    copy.start()
        for way in range(2):
            hand(way, HALF + u, span(origin(way, u // 2) + over, half_of(way, u))).wait_recv()

    done = 0
    for event in range(1, full + 1):
        u = event - 1
        kk = u // 2
        for way in range(2):
            p, h = origin(way, kk), half_of(way, u)
            hop(way, HALF + u, span(p, h)).wait_recv()
            if event <= hops and way in ways(event - 1):
                e = origin(way, event - 1)
                hop(way, event - 1, block(e)).wait_recv()
                if way in ways(event) and event < hops:
                    hop(way, event, block(e)).start()
                hand(way, event - 1, block(e)).start()
                for copy in across(slot_of(way, event - 1), e):
                    copy.start()
            if u + 2 < full:
                hop(way, HALF + u + 2, span(p, h)).start()
            elif u + 2 == full:
                for j, (first, rows) in enumerate(ROWS):
                    hop(way, LAST + j, span(p, h, first, rows)).start()
            hand(way, HALF + u, span(p, h)).start()
        from_pair(event - 1)
        if event >= 2:
            merge_event(event - 2)
            done = event - 2
    from_pair(full)
    for event in range(done + 1, full + 1):
        merge_event(event)

    wait_across([slot_of(0, hops - 1) + other for other in range(2)])
    far = origin(0, hops - 1)
    for way in range(2):
        for other in range(2):
            p = far + other * over
            unfold(2 * way + other, p, way)
            for c in range(0, width, 256):
                whole[p, pl.ds(way * half, half), c : c + 256] = jnp.dot(
                    low_n[2 * way + other], high[:, c : c + 256], preferred_element_type=F32
                )

    @pl.loop(0, count)
    def _(p):
        norms[p] = extra[p, :, 3]

    def sent(copies):
        for copy in copies:
            copy.wait_send()

    for slot in range(4 * hops):
        sent(across(slot, me))
    sent([hand(2, 0, block(me)), hand(2, 1, raw.at[me])])
    for way in range(2):
        for kk in range(hops):
            if way in ways(kk):
                sent([hop(way, kk, block(me)), hand(way, kk, block(me))])
        for u in range(full):
            sent([hand(way, HALF + u, span(me, 0))])
        for u in range(full - 2):
            sent([hop(way, HALF + u, span(me, 0))])

    def last_pair(j):
        first, rows = ROWS[j]
        for way in range(2):
            hand(way, LAST + j, span(far + over, way, first, rows)).wait_recv()
            merge(2 * way + 1, far + over, way, first, rows, True)

    for j, (first, rows) in enumerate(ROWS):
        for way in range(2):
            hop(way, LAST + j, span(far, way, first, rows)).wait_recv()
            hand(way, LAST + j, span(far, way, first, rows)).start()
        if j > 0:
            last_pair(j - 1)
        for way in range(2):
            merge(2 * way, far, way, first, rows, True)
    last_pair(len(ROWS) - 1)
    most[...] = peak[...]

    for way in range(2):
        for u in range(full - 2, full):
            sent([hop(way, HALF + u, span(me, 0))])
        for j, (first, rows) in enumerate(ROWS):
            sent([hop(way, LAST + j, span(me, 0, first, rows)), hand(way, LAST + j, span(me, 0, first, rows))])


def serve_kernel(
    whole, most, norms,
    q, k, v, scale_q, scale_k, scale_v, norm,
    q_out, k_out, v_out, scale_out, per, norm_f, norm_out,
    big_sem, sem,
):
    pieces, deep, width = whole.shape
    outs, stages = (q, k, v), (q_out, k_out, v_out)
    widths = tuple(a.shape[1] for a in outs)
    starts = (0, widths[0], widths[0] + widths[1])
    scale_out[...] = jnp.max(most[...], axis=0, keepdims=True)
    small = []
    for n, (dst, start, wide) in enumerate(zip((scale_q, scale_k, scale_v), starts, widths)):
        small.append(pltpu.make_async_copy(scale_out.at[:, pl.ds(start, wide)], dst, sem.at[n]))
    per[...] = 1.0 / scale_out[...]
    rows = 32

    def out(n, p):
        at = pl.ds(pl.multiple_of(p * deep, deep), deep)
        return pltpu.make_async_copy(stages[n].at[at], outs[n].at[at], big_sem.at[n, p])

    @pl.loop(0, pieces)
    def _(p):
        @pl.loop(0, deep // rows)
        def _(r):
            here = pl.ds(pl.multiple_of(r * rows, rows), rows)
            there = pl.ds(pl.multiple_of(p * deep + r * rows, rows), rows)
            for n in range(3):
                cols = slice(starts[n], starts[n] + widths[n])
                stages[n][there, :] = (whole[p, here, cols] * per[:, cols]).astype(BF16)

        for n in range(3):
            out(n, p).start()

    models = norms.shape[1]
    wide = norm_f.shape[1] // 2
    for m in range(0, models, 2):
        pair = jnp.concatenate(
            [norms[:, n].astype(F32)[:, 0, :wide] for n in (m, m + 1)], axis=1
        )
        norm_f[pl.ds(m // 2, pieces, stride=models // 2), :] = pair
    norm_out[...] = norm_f[...].astype(BF16)
    small.append(pltpu.make_async_copy(norm_out, norm, sem.at[3]))
    for copy in small:
        copy.start()
    for copy in small:
        copy.wait()

    @pl.loop(0, pieces)
    def _(p):
        for n in range(3):
            out(n, p).wait()


def local(count, models, q, low_q, high_q, k, low_k, high_k, v, low_v, high_v, norm_train, norm_step):
    deep, rank = low_q.shape
    widths = (q.shape[1], k.shape[1], v.shape[1])
    width = sum(widths)
    copies = count // 4 + 2 * (count // 4 - 1) + len(ROWS)
    piece = norm_train.shape[0]
    dma = pltpu.SemaphoreType.DMA
    anywhere = pl.BlockSpec(memory_space=pl.ANY)
    vmem = pl.BlockSpec(memory_space=pltpu.VMEM)
    whole, most, norms = pl.pallas_call(
        functools.partial(gather_kernel, count, models),
        out_shape=(
            pltpu.VMEM((count, deep, width), F32),
            pltpu.VMEM((8, width), F32),
            pltpu.VMEM((count, models, 8, 128), BF16),
        ),
        in_specs=[anywhere] * 11,
        out_specs=(vmem, vmem, vmem),
        scratch_shapes=[
            pltpu.VMEM((count, deep, width), BF16),
            pltpu.VMEM((count, models, 4, 8, 128), BF16),
            pltpu.VMEM((4, deep // 2, 3 * rank), BF16),
            pltpu.VMEM((3 * rank, width), BF16),
            pltpu.VMEM((2, 1, piece), F32),
            pltpu.VMEM((8, width), F32),
            dma((11,)),
            dma((count, models - 1)),
            dma((count, models - 1)),
            dma((2, copies)),
            dma((2, copies)),
            dma((3, copies)),
            dma((3, copies)),
        ],
        compiler_params=pltpu.CompilerParams(
            collective_id=0, has_side_effects=True, vmem_limit_bytes=20 * 2**20
        ),
        name="gather",
    )(
        *(
            pltpu.with_memory_space_constraint(a, pltpu.HBM)
            for a in (
                q, k, v, low_q.T, low_k.T, low_v.T, high_q, high_k, high_v,
                norm_train.reshape(1, piece), norm_step.reshape(1, piece),
            )
        )
    )
    total = count * deep
    sizes = tuple((total, w) for w in widths)
    serving_q, serving_k, serving_v, scale_q, scale_k, scale_v, norm = pl.pallas_call(
        serve_kernel,
        out_shape=tuple(jax.ShapeDtypeStruct(s, BF16) for s in sizes)
        + tuple(jax.ShapeDtypeStruct((1, w), F32) for w in widths)
        + (jax.ShapeDtypeStruct((count * models // 2, 2 * piece), BF16),),
        in_specs=[vmem] * 3,
        out_specs=(anywhere,) * 7,
        scratch_shapes=[pltpu.VMEM(s, BF16) for s in sizes]
        + [
            pltpu.VMEM((1, width), F32),
            pltpu.VMEM((1, width), F32),
            pltpu.VMEM((count * models // 2, 2 * piece), F32),
            pltpu.VMEM((count * models // 2, 2 * piece), BF16),
            dma((3, count)),
            dma((4,)),
        ],
        compiler_params=pltpu.CompilerParams(vmem_limit_bytes=20 * 2**20),
        name="serve",
    )(*(pltpu.with_memory_space_constraint(a, pltpu.VMEM) for a in (whole, most, norms)))
    return (
        serving_q, serving_k, serving_v,
        scale_q.reshape(-1), scale_k.reshape(-1), scale_v.reshape(-1), norm.reshape(-1),
    )


def solution(mesh):
    in_specs = (
        P(("unit", "shard"), "model"),
        P(("unit", "shard"), None),
        P("unit", "model"),
        P(("unit", "shard"), "model"),
        P(("unit", "shard"), None),
        P("unit", "model"),
        P(("unit", "shard"), "model"),
        P(("unit", "shard"), None),
        P("unit", "model"),
        P(("unit", "shard", "model")),
        P(("unit", "shard", "model")),
    )
    out_specs = (
        P("unit", "model"),
        P("unit", "model"),
        P("unit", "model"),
        P(("unit", "model")),
        P(("unit", "model")),
        P(("unit", "model")),
        P("unit"),
    )
    body = functools.partial(local, mesh.shape["shard"], mesh.shape["model"])
    return jax.shard_map(body, mesh=mesh, in_specs=in_specs, out_specs=out_specs, check_vma=False)
```

```python
import functools

import jax
import jax.numpy as jnp
from jax import lax
from jax.experimental import pallas as pl
from jax.experimental.pallas import tpu as pltpu
from jax.sharding import PartitionSpec as P

MESH = pl.DeviceIdType.MESH
F32, BF16 = jnp.float32, jnp.bfloat16
ROWS = ((0, 64), (64, 32), (96, 16), (112, 16))


def gather_kernel(
    count, models,
    q, k, v, low_q, low_k, low_v, high_q, high_k, high_v, norm_a, norm_b,
    whole, most, norms,
    raw, extra, mine, low_n, high, norm_in, peak,
    in_sem, y_send, y_recv, e_send, e_recv, give_send, give_recv,
    ring_send, ring_recv, pair_send, pair_recv, ready,
):
    me, my = lax.axis_index("shard"), lax.axis_index("model")
    right, left = lax.rem(me + 2, count), lax.rem(me + count - 2, count)
    core = lax.rem(me, 2)
    first_core = me - core
    partner = me + 1 - 2 * core
    over = partner - me
    lead, rest = core == 0, core == 1
    rank = low_q.shape[0]
    half = raw.shape[1] // 2
    hops = count // 4
    full = 2 * (hops - 1)
    widths = (q.shape[1], k.shape[1], v.shape[1])
    starts = (0, widths[0], widths[0] + widths[1])
    width = sum(widths)

    fetch = []
    for n, (src, start, wide) in enumerate(zip((q, k, v), starts, widths)):
        fetch.append(pltpu.make_async_copy(src, raw.at[me, :, pl.ds(start, wide)], in_sem.at[n]))
    at = (
        pl.ds(pl.multiple_of(lax.div(my, 2) * 8, 8), 8),
        pl.ds(pl.multiple_of(lax.rem(my, 2) * half, half), half),
    )

    def fetch_low(block):
        return [
            pltpu.make_async_copy(src.at[at], block.at[n], in_sem.at[3 + n])
            for n, src in enumerate((low_q, low_k, low_v))
        ]

    for n, (src, start, wide) in enumerate(zip((high_q, high_k, high_v), starts, widths)):
        fetch.append(
            pltpu.make_async_copy(src, high.at[pl.ds(n * rank, rank), pl.ds(start, wide)], in_sem.at[6 + n])
        )
    for n, src in enumerate((norm_a, norm_b)):
        fetch.append(pltpu.make_async_copy(src, norm_in.at[n], in_sem.at[9 + n]))
    for copy in fetch[6:] + fetch[:6]:
        copy.start()

    @pl.when(lead)
    def _():
        for copy in fetch_low(extra.at[my, me]):
            copy.start()

    @pl.when(rest)
    def _():
        for copy in fetch_low(mine):
            copy.start()

    barrier = pltpu.get_barrier_semaphore()

    def tell(other):
        pl.semaphore_signal(barrier, inc=1, device_id=other, device_id_type=MESH)

    for chip in (first_core + 2, first_core + count - 2):
        tell({"shard": lax.rem(chip, count) + 1})

    @pl.when(lead)
    def _():
        tell({"shard": partner})
        for step in range(1, models):
            tell({"model": lax.rem(my + step, models)})

    for copy in fetch[6:]:
        copy.wait()
    total = norm_in[0] + norm_in[1]
    spread = jnp.concatenate([total, jnp.zeros((1, 128 - total.shape[1]), F32)], axis=1)
    tile = jnp.broadcast_to(spread, (8, 128)).astype(BF16)

    @pl.when(lead)
    def _():
        extra[my, me, 3] = tile

    @pl.when(rest)
    def _():
        mine[3] = tile

    for n in range(3):
        for m in range(3):
            if n != m:
                high[n * rank : (n + 1) * rank, starts[m] : starts[m] + widths[m]] = jnp.zeros(
                    (rank, widths[m]), BF16
                )
    peak[...] = jnp.zeros_like(peak)
    for copy in fetch[:6]:
        copy.wait()

    @pl.when(lead)
    def _():
        for copy in fetch_low(extra.at[my, me]):
            copy.wait()

    @pl.when(rest)
    def _():
        for copy in fetch_low(mine):
            copy.wait()

    @pl.when(rest)
    def _():
        pl.semaphore_wait(barrier, 5)
        pl.semaphore_signal(ready, inc=1, device_id={"shard": partner}, device_id_type=MESH)

    @pl.when(lead)
    def _():
        pl.semaphore_wait(ready, 1)

    def block(chip):
        return extra.at[my, pl.ds(chip, 2)]

    def span(p, h, first=0, rows=half):
        return raw.at[p, pl.ds(pl.multiple_of(h * half + first, 16), rows)]

    def send(ref, sends, recvs, index, to):
        return pltpu.make_async_remote_copy(
            src_ref=ref, dst_ref=ref, send_sem=sends.at[index], recv_sem=recvs.at[index],
            device_id=to, device_id_type=MESH,
        )

    def hop(way, j, ref):
        return send(ref, ring_send, ring_recv, (way, j), {"shard": (right, left)[way]})

    def hand(way, j, ref):
        return send(ref, pair_send, pair_recv, (way, j), {"shard": partner})

    def pass_on(way, kk, chip):
        return send(block(chip), e_send, e_recv, (way, kk), {"shard": (right, left)[way]})

    def across(slot, chip):
        return [
            send(block(chip), y_send, y_recv, (slot, step - 1), {"model": lax.rem(my + step, models)})
            for step in range(1, models)
        ]

    def give(slot, chip):
        return send(extra.at[:, pl.ds(chip, 2)], give_send, give_recv, (slot,), {"shard": partner})

    def give_own(p):
        return pltpu.make_async_remote_copy(
            src_ref=mine, dst_ref=extra.at[my, p],
            send_sem=give_send.at[2 * hops], recv_sem=give_recv.at[2 * hops],
            device_id={"shard": partner}, device_id_type=MESH,
        )

    def origin(way, hop_count):
        far = 2 * (hop_count + 1)
        return lax.rem(me + count + (2 * way - 1) * far, count)

    def chip_of(way, hop_count):
        return origin(way, hop_count) - core

    def slot_of(way, kk):
        return 1 + kk + hops * way

    def half_of(way, u):
        return lax.rem(u + way, 2)

    LAST = full

    for way in range(2):
        hop(way, 0, span(me, way)).start()

    @pl.when(rest)
    def _():
        give_own(me).start()

    hand(2, 0, raw.at[me]).start()

    @pl.when(lead)
    def _():
        give_own(partner).wait_recv()
        for way in range(2):
            pass_on(way, 0, first_core).start()

    for way in range(2):
        hop(way, 1, span(me, 1 - way)).start()

    def unfold(slot, p, h):
        parts = [
            extra[quarter + h, p, n].astype(F32)
            for n in range(3)
            for quarter in range(0, models, 2)
        ]
        low_n[slot] = jnp.transpose(jnp.concatenate(parts, axis=0), (1, 0)).astype(BF16)

    def merge(p, h, first, rows, formed=False):
        at = pl.ds(pl.multiple_of(h * half + first, 16), rows)
        wide = 256
        for c in range(0, width, wide):
            cols = slice(c, c + wide)
            add = (
                whole[p, at, cols]
                if formed
                else jnp.dot(low_n[0], high[:, cols], preferred_element_type=F32)
            )
            new = raw[p, at, cols].astype(F32) + add
            whole[p, at, cols] = new
            peak[:, cols] = jnp.maximum(
                peak[:, cols], jnp.max(jnp.abs(new).reshape(rows // 8, 8, wide), axis=0)
            )

    def merge_four(which):
        @pl.loop(0, 4)
        def _(j):
            p, h = which(lax.div(j, 2), lax.rem(j, 2))
            unfold(0, p, h)
            merge(p, h, 0, half)

    def ways(kk):
        return range(2 if kk < hops - 1 else 1)

    def held(kk):
        return [(0, first_core)] * (kk == 0) + [(slot_of(way, kk), chip_of(way, kk)) for way in ways(kk)]

    def collect(kk):
        @pl.when(lead)
        def _():
            for slot, chip in held(kk):
                for copy in across(slot, chip):
                    copy.wait_recv()
                give(slot, chip).start()

    def given(slot, chip):
        @pl.when(rest)
        def _():
            give(slot, chip).wait_recv()

    def merge_event(event):
        if event == 0:
            given(0, first_core)
            hand(2, 0, raw.at[partner]).wait_recv()
            merge_four(lambda way, other: (me + other * over, way))
            return
        u = event - 1
        kk = u // 2
        if u % 2 == 0:
            for way in range(2):
                given(slot_of(way, kk), chip_of(way, kk))
        merge_four(lambda way, other: (origin(way, kk) + other * over, half_of(way, u)))

    def far_products():
        given(slot_of(0, hops - 1), chip_of(0, hops - 1))

        @pl.loop(0, 4)
        def _(j):
            way, other = lax.div(j, 2), lax.rem(j, 2)
            p = far + other * over
            unfold(0, p, way)
            at = pl.ds(pl.multiple_of(way * half, half), half)
            for c in range(0, width, 256):
                whole[p, at, c : c + 256] = jnp.dot(low_n[0], high[:, c : c + 256], preferred_element_type=F32)

    far = origin(0, hops - 1)
    todo = list(range(full + 1))
    for event in range(1, full + 1):
        u = event - 1
        kk = u // 2
        for way in range(2):
            p, h = origin(way, kk), half_of(way, u)
            hop(way, u, span(p, h)).wait_recv()
            if u + 2 < full:
                hop(way, u + 2, span(p, h)).start()
            elif u + 2 == full:
                for j, (first, rows) in enumerate(ROWS):
                    hop(way, LAST + j, span(p, h, first, rows)).start()
            hand(way, u, span(p, h)).start()
        if event <= hops:

            @pl.when(lead)
            def _():
                for way in ways(event - 1):
                    chip = chip_of(way, event - 1)
                    pass_on(way, event - 1, chip).wait_recv()
                    if event < hops and way in ways(event):
                        pass_on(way, event, chip).start()
                if event == 1:
                    pl.semaphore_wait(barrier, models - 1)
                for slot, chip in held(event - 1):
                    for copy in across(slot, chip):
                        copy.start()

        if 2 <= event <= hops + 1:
            collect(event - 2)
        if event >= 2:
            for way in range(2):
                hand(way, u - 1, span(origin(way, (u - 1) // 2) + over, half_of(way, u - 1))).wait_recv()
        while todo and todo[0] + (2 if event >= full - 1 else 3) <= event:
            merge_event(todo.pop(0))
        if event == full:
            if full < hops + 1:
                collect(hops - 1)
            far_products()
    for way in range(2):
        hand(way, full - 1, span(origin(way, (full - 1) // 2) + over, half_of(way, full - 1))).wait_recv()
    for event in todo:
        merge_event(event)

    @pl.loop(0, count)
    def _(p):
        norms[:, p] = extra[:, p, 3]

    def sent(copies):
        for copy in copies:
            copy.wait_send()

    @pl.when(lead)
    def _():
        for slot in range(2 * hops):
            sent(across(slot, first_core) + [give(slot, first_core)])
        for kk in range(hops):
            sent([pass_on(way, kk, first_core) for way in ways(kk)])

    @pl.when(rest)
    def _():
        sent([give_own(me)])

    sent([hand(2, 0, raw.at[me])])
    for way in range(2):
        sent([hand(way, u, span(me, 0)) for u in range(full)])
        sent([hop(way, u, span(me, 0)) for u in range(full - 2)])

    def last_pair(j):
        first, rows = ROWS[j]
        for way in range(2):
            hand(way, LAST + j, span(far + over, way, first, rows)).wait_recv()
            merge(far + over, way, first, rows, True)

    for j, (first, rows) in enumerate(ROWS):
        for way in range(2):
            hop(way, LAST + j, span(far, way, first, rows)).wait_recv()
            hand(way, LAST + j, span(far, way, first, rows)).start()
        if j > 0:
            last_pair(j - 1)
        for way in range(2):
            merge(far, way, first, rows, True)
    last_pair(len(ROWS) - 1)
    most[...] = peak[...]

    for way in range(2):
        for u in range(full - 2, full):
            sent([hop(way, u, span(me, 0))])
        for j, (first, rows) in enumerate(ROWS):
            sent([hop(way, LAST + j, span(me, 0, first, rows)), hand(way, LAST + j, span(me, 0, first, rows))])


def serve_kernel(
    whole, most, norms,
    q, k, v, scale_q, scale_k, scale_v, norm,
    q_out, k_out, v_out, scale_out, per, norm_f, norm_out,
    big_sem, sem,
):
    pieces, deep, width = whole.shape
    outs, stages = (q, k, v), (q_out, k_out, v_out)
    widths = tuple(a.shape[1] for a in outs)
    starts = (0, widths[0], widths[0] + widths[1])
    scale_out[...] = jnp.max(most[...], axis=0, keepdims=True)
    small = []
    for n, (dst, start, wide) in enumerate(zip((scale_q, scale_k, scale_v), starts, widths)):
        small.append(pltpu.make_async_copy(scale_out.at[:, pl.ds(start, wide)], dst, sem.at[n]))
    per[...] = 1.0 / scale_out[...]
    rows = 32

    def out(n, p):
        at = pl.ds(pl.multiple_of(p * deep, deep), deep)
        return pltpu.make_async_copy(stages[n].at[at], outs[n].at[at], big_sem.at[n, p])

    @pl.loop(0, pieces)
    def _(p):
        @pl.loop(0, deep // rows)
        def _(r):
            here = pl.ds(pl.multiple_of(r * rows, rows), rows)
            there = pl.ds(pl.multiple_of(p * deep + r * rows, rows), rows)
            for n in range(3):
                cols = slice(starts[n], starts[n] + widths[n])
                stages[n][there, :] = (whole[p, here, cols] * per[:, cols]).astype(BF16)

        for n in range(3):
            out(n, p).start()

    models = norms.shape[0]
    wide = norm_f.shape[1] // 2
    for m in range(0, models, 2):
        pair = jnp.concatenate(
            [norms[n].astype(F32)[:, 0, :wide] for n in (m, m + 1)], axis=1
        )
        norm_f[pl.ds(m // 2, pieces, stride=models // 2), :] = pair
    norm_out[...] = norm_f[...].astype(BF16)
    small.append(pltpu.make_async_copy(norm_out, norm, sem.at[3]))
    for copy in small:
        copy.start()
    for copy in small:
        copy.wait()

    @pl.loop(0, pieces)
    def _(p):
        for n in range(3):
            out(n, p).wait()


def local(count, models, q, low_q, high_q, k, low_k, high_k, v, low_v, high_v, norm_train, norm_step):
    deep, rank = low_q.shape
    widths = (q.shape[1], k.shape[1], v.shape[1])
    width = sum(widths)
    copies = 2 * (count // 4 - 1) + len(ROWS)
    piece = norm_train.shape[0]
    dma = pltpu.SemaphoreType.DMA
    anywhere = pl.BlockSpec(memory_space=pl.ANY)
    vmem = pl.BlockSpec(memory_space=pltpu.VMEM)
    whole, most, norms = pl.pallas_call(
        functools.partial(gather_kernel, count, models),
        out_shape=(
            pltpu.VMEM((count, deep, width), F32),
            pltpu.VMEM((8, width), F32),
            pltpu.VMEM((models, count, 8, 128), BF16),
        ),
        in_specs=[anywhere] * 11,
        out_specs=(vmem, vmem, vmem),
        scratch_shapes=[
            pltpu.VMEM((count, deep, width), BF16),
            pltpu.VMEM((models, count, 4, 8, 128), BF16),
            pltpu.VMEM((4, 8, 128), BF16),
            pltpu.VMEM((1, deep // 2, 3 * rank), BF16),
            pltpu.VMEM((3 * rank, width), BF16),
            pltpu.VMEM((2, 1, piece), F32),
            pltpu.VMEM((8, width), F32),
            dma((11,)),
            dma((count // 2, models - 1)),
            dma((count // 2, models - 1)),
            dma((2, count // 4)),
            dma((2, count // 4)),
            dma((count // 2 + 1,)),
            dma((count // 2 + 1,)),
            dma((2, copies)),
            dma((2, copies)),
            dma((3, copies)),
            dma((3, copies)),
            pltpu.SemaphoreType.REGULAR,
        ],
        compiler_params=pltpu.CompilerParams(
            collective_id=0, has_side_effects=True, vmem_limit_bytes=20 * 2**20
        ),
        name="gather",
    )(
        *(
            pltpu.with_memory_space_constraint(a, pltpu.HBM)
            for a in (
                q, k, v, low_q.T, low_k.T, low_v.T, high_q, high_k, high_v,
                norm_train.reshape(1, piece), norm_step.reshape(1, piece),
            )
        )
    )
    total = count * deep
    sizes = tuple((total, w) for w in widths)
    serving_q, serving_k, serving_v, scale_q, scale_k, scale_v, norm = pl.pallas_call(
        serve_kernel,
        out_shape=tuple(jax.ShapeDtypeStruct(s, BF16) for s in sizes)
        + tuple(jax.ShapeDtypeStruct((1, w), F32) for w in widths)
        + (jax.ShapeDtypeStruct((count * models // 2, 2 * piece), BF16),),
        in_specs=[vmem] * 3,
        out_specs=(anywhere,) * 7,
        scratch_shapes=[pltpu.VMEM(s, BF16) for s in sizes]
        + [
            pltpu.VMEM((1, width), F32),
            pltpu.VMEM((1, width), F32),
            pltpu.VMEM((count * models // 2, 2 * piece), F32),
            pltpu.VMEM((count * models // 2, 2 * piece), BF16),
            dma((3, count)),
            dma((4,)),
        ],
        compiler_params=pltpu.CompilerParams(vmem_limit_bytes=20 * 2**20),
        name="serve",
    )(*(pltpu.with_memory_space_constraint(a, pltpu.VMEM) for a in (whole, most, norms)))
    return (
        serving_q, serving_k, serving_v,
        scale_q.reshape(-1), scale_k.reshape(-1), scale_v.reshape(-1), norm.reshape(-1),
    )


def solution(mesh):
    in_specs = (
        P(("unit", "shard"), "model"),
        P(("unit", "shard"), None),
        P("unit", "model"),
        P(("unit", "shard"), "model"),
        P(("unit", "shard"), None),
        P("unit", "model"),
        P(("unit", "shard"), "model"),
        P(("unit", "shard"), None),
        P("unit", "model"),
        P(("unit", "shard", "model")),
        P(("unit", "shard", "model")),
    )
    out_specs = (
        P("unit", "model"),
        P("unit", "model"),
        P("unit", "model"),
        P(("unit", "model")),
        P(("unit", "model")),
        P(("unit", "model")),
        P("unit"),
    )
    body = functools.partial(local, mesh.shape["shard"], mesh.shape["model"])
    return jax.shard_map(body, mesh=mesh, in_specs=in_specs, out_specs=out_specs, check_vma=False)
```

```python
import functools

import jax
import jax.numpy as jnp
from jax import lax
from jax.experimental import pallas as pl
from jax.experimental.pallas import tpu as pltpu
from jax.sharding import PartitionSpec as P

MESH = pl.DeviceIdType.MESH
F32, BF16 = jnp.float32, jnp.bfloat16
ROWS = ((0, 64), (64, 32), (96, 16), (112, 16))
MOVED = 2
BLOCKS = (1, 1, 2, 4, 4, 4)


def gather_kernel(
    count, models,
    q, k, v, low_q, low_k, low_v, high_q, high_k, high_v, norm_a, norm_b,
    whole, most, norms,
    raw, extra, mine, low_n, high, norm_in, peak,
    in_sem, y_send, y_recv, e_send, e_recv, give_send, give_recv,
    ring_send, ring_recv, pair_send, pair_recv, ready,
):
    me, my = lax.axis_index("shard"), lax.axis_index("model")
    right, left = lax.rem(me + 2, count), lax.rem(me + count - 2, count)
    core = lax.rem(me, 2)
    first_core = me - core
    partner = me + 1 - 2 * core
    over = partner - me
    lead, rest = core == 0, core == 1
    rank = low_q.shape[0]
    half = raw.shape[1] // 2
    hops = count // 4
    full = 2 * (hops - 1)
    widths = (q.shape[1], k.shape[1], v.shape[1])
    starts = (0, widths[0], widths[0] + widths[1])
    width = sum(widths)

    fetch = []
    for n, (src, start, wide) in enumerate(zip((q, k, v), starts, widths)):
        fetch.append(pltpu.make_async_copy(src, raw.at[me, :, pl.ds(start, wide)], in_sem.at[n]))
    at = (
        pl.ds(pl.multiple_of(lax.div(my, 2) * 8, 8), 8),
        pl.ds(pl.multiple_of(lax.rem(my, 2) * half, half), half),
    )

    def fetch_low(block):
        return [
            pltpu.make_async_copy(src.at[at], block.at[n], in_sem.at[3 + n])
            for n, src in enumerate((low_q, low_k, low_v))
        ]

    for n, (src, start, wide) in enumerate(zip((high_q, high_k, high_v), starts, widths)):
        fetch.append(
            pltpu.make_async_copy(src, high.at[pl.ds(n * rank, rank), pl.ds(start, wide)], in_sem.at[6 + n])
        )
    for n, src in enumerate((norm_a, norm_b)):
        fetch.append(pltpu.make_async_copy(src, norm_in.at[n], in_sem.at[9 + n]))
    for copy in fetch[6:] + fetch[:6]:
        copy.start()

    @pl.when(lead)
    def _():
        for copy in fetch_low(extra.at[my, me]):
            copy.start()

    @pl.when(rest)
    def _():
        for copy in fetch_low(mine):
            copy.start()

    barrier = pltpu.get_barrier_semaphore()

    def tell(other):
        pl.semaphore_signal(barrier, inc=1, device_id=other, device_id_type=MESH)

    @pl.when(first_core != count - 2)
    def _():
        tell({"shard": lax.rem(first_core + 2, count) + 1})

    @pl.when(first_core == 0)
    def _():
        tell({"shard": count - 1})


    @pl.when(lead)
    def _():
        tell({"shard": partner})
        for step in range(1, models):
            tell({"model": lax.rem(my + step, models)})

    for copy in fetch[6:]:
        copy.wait()
    total = norm_in[0] + norm_in[1]
    spread = jnp.concatenate([total, jnp.zeros((1, 128 - total.shape[1]), F32)], axis=1)
    tile = jnp.broadcast_to(spread, (8, 128)).astype(BF16)

    @pl.when(lead)
    def _():
        extra[my, me, 3] = tile

    @pl.when(rest)
    def _():
        mine[3] = tile

    for n in range(3):
        for m in range(3):
            if n != m:
                high[n * rank : (n + 1) * rank, starts[m] : starts[m] + widths[m]] = jnp.zeros(
                    (rank, widths[m]), BF16
                )
    peak[...] = jnp.zeros_like(peak)
    for copy in fetch[:6]:
        copy.wait()

    @pl.when(lead)
    def _():
        for copy in fetch_low(extra.at[my, me]):
            copy.wait()

    @pl.when(rest)
    def _():
        for copy in fetch_low(mine):
            copy.wait()

    def say(which, other):
        pl.semaphore_signal(ready.at[which], inc=1, device_id={"shard": other}, device_id_type=MESH)

    @pl.when(rest & (first_core == 0))
    def _():
        pl.semaphore_wait(barrier, 1)

    @pl.when(rest & (first_core != 0) & (first_core != count - 2))
    def _():
        pl.semaphore_wait(barrier, 3)

    @pl.when(rest & (first_core == count - 2))
    def _():
        pl.semaphore_wait(barrier, 5)
        for other in range(2):
            say(1, other)
        say(0, partner)
        pl.semaphore_signal(ready.at[0], inc=1)

    @pl.when(rest & (first_core != 0))
    def _():
        for other in range(2):
            say(0, lax.rem(first_core + count - 2, count) + other)
        say(1, partner)
        pl.semaphore_signal(ready.at[1], inc=1)

    pl.semaphore_wait(ready.at[0], 1)

    def block(chip):
        return extra.at[my, pl.ds(chip, 2)]

    def span(p, h, first=0, rows=half):
        return raw.at[p, pl.ds(pl.multiple_of(h * half + first, 16), rows)]

    def send(ref, sends, recvs, index, to):
        return pltpu.make_async_remote_copy(
            src_ref=ref, dst_ref=ref, send_sem=sends.at[index], recv_sem=recvs.at[index],
            device_id=to, device_id_type=MESH,
        )

    def hop(way, j, ref):
        return send(ref, ring_send, ring_recv, (way, j), {"shard": (right, left)[way]})

    def hand(way, j, ref):
        return send(ref, pair_send, pair_recv, (way, j), {"shard": partner})

    def pass_on(way, kk, chip):
        return send(block(chip), e_send, e_recv, (way, kk), {"shard": (right, left)[way]})

    def across(slot, chip):
        return [
            send(block(chip), y_send, y_recv, (slot, step - 1), {"model": lax.rem(my + step, models)})
            for step in range(1, models)
        ]

    def give(slot, chip):
        return send(extra.at[:, pl.ds(chip, 2)], give_send, give_recv, (slot,), {"shard": partner})

    def give_own(p):
        return pltpu.make_async_remote_copy(
            src_ref=mine, dst_ref=extra.at[my, p],
            send_sem=give_send.at[2 * hops], recv_sem=give_recv.at[2 * hops],
            device_id={"shard": partner}, device_id_type=MESH,
        )

    def origin(way, hop_count):
        far = 2 * (hop_count + 1)
        return lax.rem(me + count + (2 * way - 1) * far, count)

    def chip_of(way, hop_count):
        return origin(way, hop_count) - core

    def slot_of(way, kk):
        return 1 + kk + hops * way

    def moved(j, ref):
        return pltpu.make_async_remote_copy(
            src_ref=ref, dst_ref=ref,
            send_sem=ring_send.at[1, LAST + len(ROWS) + j - MOVED], recv_sem=ring_recv.at[0, LAST + j],
            device_id={"shard": left}, device_id_type=MESH,
        )

    def half_of(way, u):
        return lax.rem(u + way, 2)

    LAST = full

    hop(0, 0, span(me, 0)).start()

    @pl.when(rest)
    def _():
        give_own(me).start()

    hand(2, 0, raw.at[me]).start()
    pl.semaphore_wait(ready.at[1], 1)
    hop(1, 0, span(me, 1)).start()

    @pl.when(lead)
    def _():
        give_own(partner).wait_recv()
        for way in range(2):
            pass_on(way, 0, first_core).start()

    for way in range(2):
        hop(way, 1, span(me, 1 - way)).start()

    def unfold(slot, p, h):
        parts = [
            extra[quarter + h, p, n].astype(F32)
            for n in range(3)
            for quarter in range(0, models, 2)
        ]
        low_n[slot] = jnp.transpose(jnp.concatenate(parts, axis=0), (1, 0)).astype(BF16)

    def merge(p, h, first, rows, formed=False):
        at = pl.ds(pl.multiple_of(h * half + first, 16), rows)
        wide = 256
        for c in range(0, width, wide):
            cols = slice(c, c + wide)
            add = (
                whole[p, at, cols]
                if formed
                else jnp.dot(low_n[0], high[:, cols], preferred_element_type=F32)
            )
            new = raw[p, at, cols].astype(F32) + add
            whole[p, at, cols] = new
            peak[:, cols] = jnp.maximum(
                peak[:, cols], jnp.max(jnp.abs(new).reshape(rows // 8, 8, wide), axis=0)
            )

    def merge_four(which):
        @pl.loop(0, 4)
        def _(j):
            p, h = which(lax.div(j, 2), lax.rem(j, 2))
            unfold(0, p, h)
            merge(p, h, 0, half)

    def ways(kk):
        return range(2 if kk < hops - 1 else 1)

    def held(kk):
        return [(0, first_core)] * (kk == 0) + [(slot_of(way, kk), chip_of(way, kk)) for way in ways(kk)]

    def collect(kk):
        @pl.when(lead)
        def _():
            for slot, chip in held(kk):
                for copy in across(slot, chip):
                    copy.wait_recv()
                give(slot, chip).start()

    def given(slot, chip):
        @pl.when(rest)
        def _():
            give(slot, chip).wait_recv()

    def merge_event(event):
        if event == 0:
            given(0, first_core)
            hand(2, 0, raw.at[partner]).wait_recv()
            merge_four(lambda way, other: (me + other * over, way))
            return
        u = event - 1
        kk = u // 2
        if u % 2 == 0:
            for way in range(2):
                given(slot_of(way, kk), chip_of(way, kk))
        merge_four(lambda way, other: (origin(way, kk) + other * over, half_of(way, u)))

    def far_products():
        given(slot_of(0, hops - 1), chip_of(0, hops - 1))

        @pl.loop(0, 4)
        def _(j):
            way, other = lax.div(j, 2), lax.rem(j, 2)
            p = far + other * over
            unfold(0, p, way)
            at = pl.ds(pl.multiple_of(way * half, half), half)
            for c in range(0, width, 256):
                whole[p, at, c : c + 256] = jnp.dot(low_n[0], high[:, c : c + 256], preferred_element_type=F32)

    far = origin(0, hops - 1)
    todo = list(range(full + 1))
    for event in range(1, full + 1):
        u = event - 1
        kk = u // 2
        for way in range(2):
            p, h = origin(way, kk), half_of(way, u)
            hop(way, u, span(p, h)).wait_recv()
            if u + 2 < full:
                hop(way, u + 2, span(p, h)).start()
            elif u + 2 == full:
                for j, (first, rows) in enumerate(ROWS):
                    if way == 0 and j >= MOVED:

                        @pl.when(first_core != count - 2)
                        def _():
                            hop(way, LAST + j, span(p, h, first, rows)).start()

                    else:
                        hop(way, LAST + j, span(p, h, first, rows)).start()
            if u + 1 == full and way == 1:

                @pl.when(first_core == 2)
                def _():
                    for j in range(MOVED, len(ROWS)):
                        moved(j, span(p, h, *ROWS[j])).start()

            hand(way, u, span(p, h)).start()
        if event <= hops:

            @pl.when(lead)
            def _():
                for way in ways(event - 1):
                    chip = chip_of(way, event - 1)
                    pass_on(way, event - 1, chip).wait_recv()
                    if event < hops and way in ways(event):
                        pass_on(way, event, chip).start()
                if event == 1:
                    pl.semaphore_wait(barrier, models - 1)
                for slot, chip in held(event - 1):
                    for copy in across(slot, chip):
                        copy.start()

        if 2 <= event <= hops + 1:
            collect(event - 2)
        if event >= 2:
            for way in range(2):
                hand(way, u - 1, span(origin(way, (u - 1) // 2) + over, half_of(way, u - 1))).wait_recv()
        while todo and todo[0] + (1 if event >= full - 1 else 2) <= event and event >= 3:
            merge_event(todo.pop(0))
        if event == max(full - 1, hops + 1):
            far_products()
    for way in range(2):
        hand(way, full - 1, span(origin(way, (full - 1) // 2) + over, half_of(way, full - 1))).wait_recv()
    for event in todo:
        merge_event(event)

    @pl.loop(0, count)
    def _(p):
        norms[:, p] = extra[:, p, 3]

    def sent(copies):
        for copy in copies:
            copy.wait_send()

    @pl.when(lead)
    def _():
        for slot in range(2 * hops):
            sent(across(slot, first_core) + [give(slot, first_core)])
        for kk in range(hops):
            sent([pass_on(way, kk, first_core) for way in ways(kk)])

    @pl.when(rest)
    def _():
        sent([give_own(me)])

    sent([hand(2, 0, raw.at[me])])
    for way in range(2):
        sent([hand(way, u, span(me, 0)) for u in range(full)])
        sent([hop(way, u, span(me, 0)) for u in range(full - 2)])

    def last_pair(j):
        first, rows = ROWS[j]
        for way in range(2):
            hand(way, LAST + j, span(far + over, way, first, rows)).wait_recv()
            merge(far + over, way, first, rows, True)

    for j, (first, rows) in enumerate(ROWS):
        for way in range(2):
            hop(way, LAST + j, span(far, way, first, rows)).wait_recv()
            hand(way, LAST + j, span(far, way, first, rows)).start()
        if j > 0:
            last_pair(j - 1)
        for way in range(2):
            merge(far, way, first, rows, True)
    last_pair(len(ROWS) - 1)
    most[...] = peak[...]

    for way in range(2):
        for u in range(full - 2, full):
            sent([hop(way, u, span(me, 0))])
        for j, (first, rows) in enumerate(ROWS):
            sent([hand(way, LAST + j, span(me, 0, first, rows))])
            if way == 1 or j < MOVED:
                sent([hop(way, LAST + j, span(me, 0, first, rows))])

    @pl.when(first_core != count - 2)
    def _():
        sent([hop(0, LAST + j, span(me, 0, *ROWS[j])) for j in range(MOVED, len(ROWS))])

    @pl.when(first_core == 2)
    def _():
        sent([moved(j, span(me, 0, *ROWS[j])) for j in range(MOVED, len(ROWS))])


def serve_kernel(
    whole, most, norms,
    q, k, v, scale_q, scale_k, scale_v, norm,
    q_out, k_out, v_out, scale_out, per, norm_f, norm_out,
    big_sem, sem,
):
    pieces, deep, width = whole.shape
    outs, stages = (q, k, v), (q_out, k_out, v_out)
    widths = tuple(a.shape[1] for a in outs)
    starts = (0, widths[0], widths[0] + widths[1])
    scale_out[...] = jnp.max(most[...], axis=0, keepdims=True)
    small = []
    for n, (dst, start, wide) in enumerate(zip((scale_q, scale_k, scale_v), starts, widths)):
        small.append(pltpu.make_async_copy(scale_out.at[:, pl.ds(start, wide)], dst, sem.at[n]))
    per[...] = 1.0 / scale_out[...]
    rows = 32

    ends = [sum(BLOCKS[:b]) for b in range(len(BLOCKS) + 1)]

    def out(n, b):
        at = pl.ds(ends[b] * deep, BLOCKS[b] * deep)
        return pltpu.make_async_copy(stages[n].at[at], outs[n].at[at], big_sem.at[n, b])

    for b in range(len(BLOCKS)):

        @pl.loop(ends[b], ends[b + 1])
        def _(p):
            @pl.loop(0, deep // rows)
            def _(r):
                here = pl.ds(pl.multiple_of(r * rows, rows), rows)
                there = pl.ds(pl.multiple_of(p * deep + r * rows, rows), rows)
                for n in range(3):
                    cols = slice(starts[n], starts[n] + widths[n])
                    stages[n][there, :] = (whole[p, here, cols] * per[:, cols]).astype(BF16)

        for n in range(3):
            out(n, b).start()

    models = norms.shape[0]
    wide = norm_f.shape[1] // 2
    for m in range(0, models, 2):
        pair = jnp.concatenate(
            [norms[n].astype(F32)[:, 0, :wide] for n in (m, m + 1)], axis=1
        )
        norm_f[pl.ds(m // 2, pieces, stride=models // 2), :] = pair
    norm_out[...] = norm_f[...].astype(BF16)
    small.append(pltpu.make_async_copy(norm_out, norm, sem.at[3]))
    for copy in small:
        copy.start()
    for copy in small:
        copy.wait()

    for b in range(len(BLOCKS)):
        for n in range(3):
            out(n, b).wait()


def local(count, models, q, low_q, high_q, k, low_k, high_k, v, low_v, high_v, norm_train, norm_step):
    deep, rank = low_q.shape
    widths = (q.shape[1], k.shape[1], v.shape[1])
    width = sum(widths)
    copies = 2 * (count // 4 - 1) + len(ROWS)
    piece = norm_train.shape[0]
    dma = pltpu.SemaphoreType.DMA
    anywhere = pl.BlockSpec(memory_space=pl.ANY)
    vmem = pl.BlockSpec(memory_space=pltpu.VMEM)
    whole, most, norms = pl.pallas_call(
        functools.partial(gather_kernel, count, models),
        out_shape=(
            pltpu.VMEM((count, deep, width), F32),
            pltpu.VMEM((8, width), F32),
            pltpu.VMEM((models, count, 8, 128), BF16),
        ),
        in_specs=[anywhere] * 11,
        out_specs=(vmem, vmem, vmem),
        scratch_shapes=[
            pltpu.VMEM((count, deep, width), BF16),
            pltpu.VMEM((models, count, 4, 8, 128), BF16),
            pltpu.VMEM((4, 8, 128), BF16),
            pltpu.VMEM((1, deep // 2, 3 * rank), BF16),
            pltpu.VMEM((3 * rank, width), BF16),
            pltpu.VMEM((2, 1, piece), F32),
            pltpu.VMEM((8, width), F32),
            dma((11,)),
            dma((count // 2, models - 1)),
            dma((count // 2, models - 1)),
            dma((2, count // 4)),
            dma((2, count // 4)),
            dma((count // 2 + 1,)),
            dma((count // 2 + 1,)),
            dma((2, copies + len(ROWS) - MOVED)),
            dma((2, copies)),
            dma((3, copies)),
            dma((3, copies)),
            pltpu.SemaphoreType.REGULAR((2,)),
        ],
        compiler_params=pltpu.CompilerParams(
            collective_id=0, has_side_effects=True, vmem_limit_bytes=20 * 2**20
        ),
        name="gather",
    )(
        *(
            pltpu.with_memory_space_constraint(a, pltpu.HBM)
            for a in (
                q, k, v, low_q.T, low_k.T, low_v.T, high_q, high_k, high_v,
                norm_train.reshape(1, piece), norm_step.reshape(1, piece),
            )
        )
    )
    total = count * deep
    sizes = tuple((total, w) for w in widths)
    serving_q, serving_k, serving_v, scale_q, scale_k, scale_v, norm = pl.pallas_call(
        serve_kernel,
        out_shape=tuple(jax.ShapeDtypeStruct(s, BF16) for s in sizes)
        + tuple(jax.ShapeDtypeStruct((1, w), F32) for w in widths)
        + (jax.ShapeDtypeStruct((count * models // 2, 2 * piece), BF16),),
        in_specs=[vmem] * 3,
        out_specs=(anywhere,) * 7,
        scratch_shapes=[pltpu.VMEM(s, BF16) for s in sizes]
        + [
            pltpu.VMEM((1, width), F32),
            pltpu.VMEM((1, width), F32),
            pltpu.VMEM((count * models // 2, 2 * piece), F32),
            pltpu.VMEM((count * models // 2, 2 * piece), BF16),
            dma((3, len(BLOCKS))),
            dma((4,)),
        ],
        compiler_params=pltpu.CompilerParams(vmem_limit_bytes=20 * 2**20),
        name="serve",
    )(*(pltpu.with_memory_space_constraint(a, pltpu.VMEM) for a in (whole, most, norms)))
    return (
        serving_q, serving_k, serving_v,
        scale_q.reshape(-1), scale_k.reshape(-1), scale_v.reshape(-1), norm.reshape(-1),
    )


def solution(mesh):
    in_specs = (
        P(("unit", "shard"), "model"),
        P(("unit", "shard"), None),
        P("unit", "model"),
        P(("unit", "shard"), "model"),
        P(("unit", "shard"), None),
        P("unit", "model"),
        P(("unit", "shard"), "model"),
        P(("unit", "shard"), None),
        P("unit", "model"),
        P(("unit", "shard", "model")),
        P(("unit", "shard", "model")),
    )
    out_specs = (
        P("unit", "model"),
        P("unit", "model"),
        P("unit", "model"),
        P(("unit", "model")),
        P(("unit", "model")),
        P(("unit", "model")),
        P("unit"),
    )
    body = functools.partial(local, mesh.shape["shard"], mesh.shape["model"])
    return jax.shard_map(body, mesh=mesh, in_specs=in_specs, out_specs=out_specs, check_vma=False)
```

```python
import functools

import jax
import jax.numpy as jnp
from jax import lax
from jax.experimental import pallas as pl
from jax.experimental.pallas import tpu as pltpu
from jax.sharding import PartitionSpec as P

MESH = pl.DeviceIdType.MESH
F32, BF16 = jnp.float32, jnp.bfloat16
ROWS = ((0, 128), (128, 64), (192, 32), (224, 32))
MOVED = 2
BLOCKS = (1, 1, 2, 4, 4, 4)


def gather_kernel(
    count, models,
    q, k, v, low_q, low_k, low_v, high_q, high_k, high_v, norm_a, norm_b,
    whole, most, norms,
    raw, extra, mine, low_n, high, norm_in, peak,
    in_sem, y_send, y_recv, e_send, e_recv, give_send, give_recv,
    ring_send, ring_recv, pair_send, pair_recv, ready,
):
    me, my = lax.axis_index("shard"), lax.axis_index("model")
    right, left = lax.rem(me + 2, count), lax.rem(me + count - 2, count)
    core = lax.rem(me, 2)
    first_core = me - core
    partner = me + 1 - 2 * core
    over = partner - me
    lead, rest = core == 0, core == 1
    rank = low_q.shape[0]
    half = raw.shape[1] // 2
    hops = count // 4
    deep = raw.shape[1]
    LAST = 3 * (hops - 1)
    widths = (q.shape[1], k.shape[1], v.shape[1])
    starts = (0, widths[0], widths[0] + widths[1])
    width = sum(widths)

    fetch = []
    for n, (src, start, wide) in enumerate(zip((q, k, v), starts, widths)):
        fetch.append(pltpu.make_async_copy(src, raw.at[me, :, pl.ds(start, wide)], in_sem.at[n]))
    at = (
        pl.ds(pl.multiple_of(lax.div(my, 2) * 8, 8), 8),
        pl.ds(pl.multiple_of(lax.rem(my, 2) * half, half), half),
    )

    def fetch_low(block):
        return [
            pltpu.make_async_copy(src.at[at], block.at[n], in_sem.at[3 + n])
            for n, src in enumerate((low_q, low_k, low_v))
        ]

    for n, (src, start, wide) in enumerate(zip((high_q, high_k, high_v), starts, widths)):
        fetch.append(
            pltpu.make_async_copy(src, high.at[pl.ds(n * rank, rank), pl.ds(start, wide)], in_sem.at[6 + n])
        )
    for n, src in enumerate((norm_a, norm_b)):
        fetch.append(pltpu.make_async_copy(src, norm_in.at[n], in_sem.at[9 + n]))
    for copy in fetch[6:] + fetch[:6]:
        copy.start()

    @pl.when(lead)
    def _():
        for copy in fetch_low(extra.at[my, me]):
            copy.start()

    @pl.when(rest)
    def _():
        for copy in fetch_low(mine):
            copy.start()

    barrier = pltpu.get_barrier_semaphore()

    def tell(other):
        pl.semaphore_signal(barrier, inc=1, device_id=other, device_id_type=MESH)

    @pl.when(first_core != count - 2)
    def _():
        tell({"shard": lax.rem(first_core + 2, count) + 1})

    @pl.when(first_core == 0)
    def _():
        tell({"shard": count - 1})


    @pl.when(lead)
    def _():
        tell({"shard": partner})
        for step in range(1, models):
            tell({"model": lax.rem(my + step, models)})

    for copy in fetch[6:]:
        copy.wait()
    total = norm_in[0] + norm_in[1]
    spread = jnp.concatenate([total, jnp.zeros((1, 128 - total.shape[1]), F32)], axis=1)
    tile = jnp.broadcast_to(spread, (8, 128)).astype(BF16)

    @pl.when(lead)
    def _():
        extra[my, me, 3] = tile

    @pl.when(rest)
    def _():
        mine[3] = tile

    for n in range(3):
        for m in range(3):
            if n != m:
                high[n * rank : (n + 1) * rank, starts[m] : starts[m] + widths[m]] = jnp.zeros(
                    (rank, widths[m]), BF16
                )
    peak[...] = jnp.zeros_like(peak)
    for copy in fetch[:6]:
        copy.wait()

    @pl.when(lead)
    def _():
        for copy in fetch_low(extra.at[my, me]):
            copy.wait()

    @pl.when(rest)
    def _():
        for copy in fetch_low(mine):
            copy.wait()

    def say(which, other):
        pl.semaphore_signal(ready.at[which], inc=1, device_id={"shard": other}, device_id_type=MESH)

    @pl.when(rest & (first_core == 0))
    def _():
        pl.semaphore_wait(barrier, 1)

    @pl.when(rest & (first_core != 0) & (first_core != count - 2))
    def _():
        pl.semaphore_wait(barrier, 3)

    @pl.when(rest & (first_core == count - 2))
    def _():
        pl.semaphore_wait(barrier, 5)
        for other in range(2):
            say(1, other)
        say(0, partner)
        pl.semaphore_signal(ready.at[0], inc=1)

    @pl.when(rest & (first_core != 0))
    def _():
        for other in range(2):
            say(0, lax.rem(first_core + count - 2, count) + other)
        say(1, partner)
        pl.semaphore_signal(ready.at[1], inc=1)

    pl.semaphore_wait(ready.at[0], 1)

    def block(chip):
        return extra.at[my, pl.ds(chip, 2)]

    def span(p, first=0, rows=deep):
        return raw.at[p, pl.ds(first, rows)]

    def send(ref, sends, recvs, index, to):
        return pltpu.make_async_remote_copy(
            src_ref=ref, dst_ref=ref, send_sem=sends.at[index], recv_sem=recvs.at[index],
            device_id=to, device_id_type=MESH,
        )

    def hop(way, j, ref):
        return send(ref, ring_send, ring_recv, (way, j), {"shard": (right, left)[way]})

    def hand(way, j, ref):
        return send(ref, pair_send, pair_recv, (way, j), {"shard": partner})

    def pass_on(way, kk, chip):
        return send(block(chip), e_send, e_recv, (way, kk), {"shard": (right, left)[way]})

    def across(slot, chip):
        return [
            send(block(chip), y_send, y_recv, (slot, step - 1), {"model": lax.rem(my + step, models)})
            for step in range(1, models)
        ]

    def give(slot, chip):
        return send(extra.at[:, pl.ds(chip, 2)], give_send, give_recv, (slot,), {"shard": partner})

    def give_own(p):
        return pltpu.make_async_remote_copy(
            src_ref=mine, dst_ref=extra.at[my, p],
            send_sem=give_send.at[2 * hops], recv_sem=give_recv.at[2 * hops],
            device_id={"shard": partner}, device_id_type=MESH,
        )

    def chip_of(way, kk):
        far = 2 * (kk + 1)
        return lax.rem(first_core + count + (2 * way - 1) * far, count)

    def slot_of(way, kk):
        return 1 + kk + hops * way

    def moved(j, ref):
        return pltpu.make_async_remote_copy(
            src_ref=ref, dst_ref=ref,
            send_sem=ring_send.at[1, LAST + len(ROWS) + j - MOVED], recv_sem=ring_recv.at[0, LAST + j],
            device_id={"shard": left}, device_id_type=MESH,
        )

    def ways(kk):
        return range(2 if kk < hops - 1 else 1)

    hand(2, 0, raw.at[me]).start()

    @pl.when(rest)
    def _():
        hop(0, 0, span(me)).start()
        give_own(me).start()
        pl.semaphore_wait(ready.at[1], 1)
        hop(1, 0, span(me, 0, half)).start()
        hand(2, 0, raw.at[partner]).wait_recv()
        for way in range(2):
            hop(way, 1, span(partner)).start()
        hop(1, 2, span(me, half, half)).start()

    @pl.when(lead)
    def _():
        give_own(partner).wait_recv()
        pass_on(0, 0, first_core).start()
        pl.semaphore_wait(ready.at[1], 1)
        pass_on(1, 0, first_core).start()
        slots = [(0, first_core)]
        for kk in range(hops):
            for way in ways(kk):
                chip = chip_of(way, kk)
                pass_on(way, kk, chip).wait_recv()
                if kk + 1 < hops and way in ways(kk + 1):
                    pass_on(way, kk + 1, chip).start()
                slots.append((slot_of(way, kk), chip))
        pl.semaphore_wait(barrier, models - 1)
        for slot, chip in slots:
            for copy in across(slot, chip):
                copy.start()
        for slot, chip in slots:
            for copy in across(slot, chip):
                copy.wait_recv()
            give(slot, chip).start()

    def unfold(slot, p, h):
        parts = [
            extra[quarter + h, p, n].astype(F32)
            for n in range(3)
            for quarter in range(0, models, 2)
        ]
        low_n[slot] = jnp.transpose(jnp.concatenate(parts, axis=0), (1, 0)).astype(BF16)

    def merge(p, first, rows, formed=False):
        at = pl.ds(pl.multiple_of(first, 16), rows)
        wide = 256
        for c in range(0, width, wide):
            cols = slice(c, c + wide)
            add = (
                whole[p, at, cols]
                if formed
                else jnp.dot(low_n[0], high[:, cols], preferred_element_type=F32)
            )
            new = raw[p, at, cols].astype(F32) + add
            whole[p, at, cols] = new
            peak[:, cols] = jnp.maximum(
                peak[:, cols], jnp.max(jnp.abs(new).reshape(rows // 8, 8, wide), axis=0)
            )

    def merge_some(number, which):
        @pl.loop(0, number)
        def _(n):
            p, h = which(n)
            unfold(0, p, h)
            merge(p, h * half, half)

    def given(slots):
        @pl.when(rest)
        def _():
            for slot in slots:
                give(slot, first_core).wait_recv()

    PARTS = (
        ((0, 1, 0, deep), (1, 1, 0, half)),
        ((1, 0, 0, deep),),
        ((0, 0, 0, deep), (1, 1, half, half)),
    )
    INDEX = (((0, 2, 0), (1, 3, 0)), ((1, 3, 1),), ((0, 2, 1), (1, 3, 2)))

    def merge_part(kk, part):
        chips = chip_of(0, kk), chip_of(1, kk)

        def way_chip(way):
            return chips[0] + way * (chips[1] - chips[0])

        if part == 0:
            given([slot_of(way, kk) for way in range(2)])
            merge_some(3, lambda n: (way_chip(lax.div(n, 2)) + 1, lax.rem(n, 2)))
        elif part == 1:
            merge_some(2, lambda n: (chips[1], n))
        else:
            merge_some(3, lambda n: (way_chip(lax.div(n, 2)) + lax.div(n, 2), lax.div(n + 1, 2)))

    def merge_own():
        given([0])

        @pl.when(lead)
        def _():
            hand(2, 0, raw.at[partner]).wait_recv()

        merge_some(4, lambda n: (first_core + lax.div(n, 2), lax.rem(n, 2)))

    far = chip_of(0, hops - 1)

    def far_products():
        given([slot_of(0, hops - 1)])

        @pl.loop(0, 4)
        def _(n):
            p, h = far + lax.div(n, 2), lax.rem(n, 2)
            unfold(0, p, h)
            at = pl.ds(pl.multiple_of(h * half, half), half)
            for c in range(0, width, 256):
                whole[p, at, c : c + 256] = jnp.dot(low_n[0], high[:, c : c + 256], preferred_element_type=F32)

    todo = [merge_own]
    events = [(kk, part) for kk in range(hops - 1) for part in range(3)]
    for e, (kk, part) in enumerate(events):
        last = kk == hops - 2

        @pl.when(rest)
        def _():
            for (way, piece, first, rows), (_, per_chip, place) in zip(PARTS[part], INDEX[part]):
                p, n = chip_of(way, kk) + piece, per_chip * kk + place
                hop(way, n, span(p, first, rows)).wait_recv()
                if not last:
                    hop(way, n + per_chip, span(p, first, rows)).start()
                elif piece != way:
                    for j, rows_j in enumerate(ROWS):
                        if way == 0 and j >= MOVED:

                            @pl.when(first_core != count - 2)
                            def _():
                                hop(way, LAST + j, span(p, *rows_j)).start()

                        else:
                            hop(way, LAST + j, span(p, *rows_j)).start()
                elif way == 1 and part == 2:

                    @pl.when(first_core == 2)
                    def _():
                        for j in range(MOVED, len(ROWS)):
                            moved(j, span(p, *ROWS[j])).start()

                hand(way, n, span(p, first, rows)).start()

        if e >= 2:
            todo.pop(0)()
        if e >= 4 and len(todo) > 1:
            todo.pop(0)()
        if e == len(events) - 2:
            far_products()

        @pl.when(lead)
        def _():
            for (way, piece, first, rows), (_, per_chip, place) in zip(PARTS[part], INDEX[part]):
                hand(way, per_chip * kk + place, span(chip_of(way, kk) + piece, first, rows)).wait_recv()

        todo.append(functools.partial(merge_part, kk, part))
    for task in todo:
        task()

    @pl.loop(0, count)
    def _(p):
        norms[:, p] = extra[:, p, 3]

    def sent(copies):
        for copy in copies:
            copy.wait_send()

    @pl.when(lead)
    def _():
        for slot in range(2 * hops):
            sent(across(slot, first_core) + [give(slot, first_core)])
        for kk in range(hops):
            sent([pass_on(way, kk, first_core) for way in ways(kk)])

    @pl.when(rest)
    def _():
        sent([give_own(me)])
        for kk, part in events:
            for (way, piece, first, rows), (_, per_chip, place) in zip(PARTS[part], INDEX[part]):
                n = per_chip * kk + place
                sent([hand(way, n, span(me, first, rows)), hop(way, n, span(me, first, rows))])

    sent([hand(2, 0, raw.at[me])])
    for j, (first, rows) in enumerate(ROWS):

        @pl.when(rest)
        def _():
            for way in range(2):
                hop(way, LAST + j, span(far + 1 - way, first, rows)).wait_recv()
                hand(way, LAST + j, span(far + 1 - way, first, rows)).start()

        @pl.when(lead)
        def _():
            for way in range(2):
                hand(way, LAST + j, span(far + 1 - way, first, rows)).wait_recv()

        for way in range(2):
            merge(far + 1 - way, first, rows, True)
    most[...] = peak[...]

    @pl.when(rest)
    def _():
        for way in range(2):
            for j, (first, rows) in enumerate(ROWS):
                sent([hand(way, LAST + j, span(me, first, rows))])
                if way == 1 or j < MOVED:
                    sent([hop(way, LAST + j, span(me, first, rows))])

    @pl.when(rest & (first_core != count - 2))
    def _():
        sent([hop(0, LAST + j, span(me, *ROWS[j])) for j in range(MOVED, len(ROWS))])

    @pl.when(rest & (first_core == 2))
    def _():
        sent([moved(j, span(me, *ROWS[j])) for j in range(MOVED, len(ROWS))])


def serve_kernel(
    whole, most, norms,
    q, k, v, scale_q, scale_k, scale_v, norm,
    q_out, k_out, v_out, scale_out, per, norm_f, norm_out,
    big_sem, sem,
):
    pieces, deep, width = whole.shape
    outs, stages = (q, k, v), (q_out, k_out, v_out)
    widths = tuple(a.shape[1] for a in outs)
    starts = (0, widths[0], widths[0] + widths[1])
    scale_out[...] = jnp.max(most[...], axis=0, keepdims=True)
    small = []
    for n, (dst, start, wide) in enumerate(zip((scale_q, scale_k, scale_v), starts, widths)):
        small.append(pltpu.make_async_copy(scale_out.at[:, pl.ds(start, wide)], dst, sem.at[n]))
    per[...] = 1.0 / scale_out[...]
    rows = 32

    ends = [sum(BLOCKS[:b]) for b in range(len(BLOCKS) + 1)]

    def out(n, b):
        at = pl.ds(ends[b] * deep, BLOCKS[b] * deep)
        return pltpu.make_async_copy(stages[n].at[at], outs[n].at[at], big_sem.at[n, b])

    for b in range(len(BLOCKS)):

        @pl.loop(ends[b], ends[b + 1])
        def _(p):
            @pl.loop(0, deep // rows)
            def _(r):
                here = pl.ds(pl.multiple_of(r * rows, rows), rows)
                there = pl.ds(pl.multiple_of(p * deep + r * rows, rows), rows)
                for n in range(3):
                    cols = slice(starts[n], starts[n] + widths[n])
                    stages[n][there, :] = (whole[p, here, cols] * per[:, cols]).astype(BF16)

        for n in range(3):
            out(n, b).start()

    models = norms.shape[0]
    wide = norm_f.shape[1] // 2
    for m in range(0, models, 2):
        pair = jnp.concatenate(
            [norms[n].astype(F32)[:, 0, :wide] for n in (m, m + 1)], axis=1
        )
        norm_f[pl.ds(m // 2, pieces, stride=models // 2), :] = pair
    norm_out[...] = norm_f[...].astype(BF16)
    small.append(pltpu.make_async_copy(norm_out, norm, sem.at[3]))
    for copy in small:
        copy.start()
    for copy in small:
        copy.wait()

    for b in range(len(BLOCKS)):
        for n in range(3):
            out(n, b).wait()


def local(count, models, q, low_q, high_q, k, low_k, high_k, v, low_v, high_v, norm_train, norm_step):
    deep, rank = low_q.shape
    widths = (q.shape[1], k.shape[1], v.shape[1])
    width = sum(widths)
    copies = 3 * (count // 4 - 1) + len(ROWS)
    piece = norm_train.shape[0]
    dma = pltpu.SemaphoreType.DMA
    anywhere = pl.BlockSpec(memory_space=pl.ANY)
    vmem = pl.BlockSpec(memory_space=pltpu.VMEM)
    whole, most, norms = pl.pallas_call(
        functools.partial(gather_kernel, count, models),
        out_shape=(
            pltpu.VMEM((count, deep, width), F32),
            pltpu.VMEM((8, width), F32),
            pltpu.VMEM((models, count, 8, 128), BF16),
        ),
        in_specs=[anywhere] * 11,
        out_specs=(vmem, vmem, vmem),
        scratch_shapes=[
            pltpu.VMEM((count, deep, width), BF16),
            pltpu.VMEM((models, count, 4, 8, 128), BF16),
            pltpu.VMEM((4, 8, 128), BF16),
            pltpu.VMEM((1, deep // 2, 3 * rank), BF16),
            pltpu.VMEM((3 * rank, width), BF16),
            pltpu.VMEM((2, 1, piece), F32),
            pltpu.VMEM((8, width), F32),
            dma((11,)),
            dma((count // 2, models - 1)),
            dma((count // 2, models - 1)),
            dma((2, count // 4)),
            dma((2, count // 4)),
            dma((count // 2 + 1,)),
            dma((count // 2 + 1,)),
            dma((2, copies + len(ROWS) - MOVED)),
            dma((2, copies)),
            dma((3, copies)),
            dma((3, copies)),
            pltpu.SemaphoreType.REGULAR((2,)),
        ],
        compiler_params=pltpu.CompilerParams(
            collective_id=0, has_side_effects=True, vmem_limit_bytes=20 * 2**20
        ),
        name="gather",
    )(
        *(
            pltpu.with_memory_space_constraint(a, pltpu.HBM)
            for a in (
                q, k, v, low_q.T, low_k.T, low_v.T, high_q, high_k, high_v,
                norm_train.reshape(1, piece), norm_step.reshape(1, piece),
            )
        )
    )
    total = count * deep
    sizes = tuple((total, w) for w in widths)
    serving_q, serving_k, serving_v, scale_q, scale_k, scale_v, norm = pl.pallas_call(
        serve_kernel,
        out_shape=tuple(jax.ShapeDtypeStruct(s, BF16) for s in sizes)
        + tuple(jax.ShapeDtypeStruct((1, w), F32) for w in widths)
        + (jax.ShapeDtypeStruct((count * models // 2, 2 * piece), BF16),),
        in_specs=[vmem] * 3,
        out_specs=(anywhere,) * 7,
        scratch_shapes=[pltpu.VMEM(s, BF16) for s in sizes]
        + [
            pltpu.VMEM((1, width), F32),
            pltpu.VMEM((1, width), F32),
            pltpu.VMEM((count * models // 2, 2 * piece), F32),
            pltpu.VMEM((count * models // 2, 2 * piece), BF16),
            dma((3, len(BLOCKS))),
            dma((4,)),
        ],
        compiler_params=pltpu.CompilerParams(vmem_limit_bytes=20 * 2**20),
        name="serve",
    )(*(pltpu.with_memory_space_constraint(a, pltpu.VMEM) for a in (whole, most, norms)))
    return (
        serving_q, serving_k, serving_v,
        scale_q.reshape(-1), scale_k.reshape(-1), scale_v.reshape(-1), norm.reshape(-1),
    )


def solution(mesh):
    in_specs = (
        P(("unit", "shard"), "model"),
        P(("unit", "shard"), None),
        P("unit", "model"),
        P(("unit", "shard"), "model"),
        P(("unit", "shard"), None),
        P("unit", "model"),
        P(("unit", "shard"), "model"),
        P(("unit", "shard"), None),
        P("unit", "model"),
        P(("unit", "shard", "model")),
        P(("unit", "shard", "model")),
    )
    out_specs = (
        P("unit", "model"),
        P("unit", "model"),
        P("unit", "model"),
        P(("unit", "model")),
        P(("unit", "model")),
        P(("unit", "model")),
        P("unit"),
    )
    body = functools.partial(local, mesh.shape["shard"], mesh.shape["model"])
    return jax.shard_map(body, mesh=mesh, in_specs=in_specs, out_specs=out_specs, check_vma=False)
```

```python
import functools

import jax
import jax.numpy as jnp
from jax import lax
from jax.experimental import pallas as pl
from jax.experimental.pallas import tpu as pltpu
from jax.sharding import PartitionSpec as P

MESH = pl.DeviceIdType.MESH
F32, BF16 = jnp.float32, jnp.bfloat16
ROWS = ((0, 128), (128, 64), (192, 32), (224, 32))
MOVED = 3
BLOCKS = (1, 1, 2, 4, 4, 4)


def gather_kernel(
    count, models,
    q, k, v, low_q, low_k, low_v, high_q, high_k, high_v, norm_a, norm_b,
    whole, most, norms,
    raw, extra, mine, low_n, high, norm_in, peak,
    in_sem, y_send, y_recv, e_send, e_recv, give_send, give_recv,
    ring_send, ring_recv, pair_send, pair_recv, ready,
):
    me, my = lax.axis_index("shard"), lax.axis_index("model")
    right, left = lax.rem(me + 2, count), lax.rem(me + count - 2, count)
    core = lax.rem(me, 2)
    first_core = me - core
    partner = me + 1 - 2 * core
    over = partner - me
    lead, rest = core == 0, core == 1
    rank = low_q.shape[0]
    half = raw.shape[1] // 2
    hops = count // 4
    deep = raw.shape[1]
    LAST = 3 * (hops - 1)
    widths = (q.shape[1], k.shape[1], v.shape[1])
    starts = (0, widths[0], widths[0] + widths[1])
    width = sum(widths)

    fetch = []
    for n, (src, start, wide) in enumerate(zip((q, k, v), starts, widths)):
        fetch.append(pltpu.make_async_copy(src, raw.at[me, :, pl.ds(start, wide)], in_sem.at[n]))
    at = (
        pl.ds(pl.multiple_of(lax.div(my, 2) * 8, 8), 8),
        pl.ds(pl.multiple_of(lax.rem(my, 2) * half, half), half),
    )

    def fetch_low(block):
        return [
            pltpu.make_async_copy(src.at[at], block.at[n], in_sem.at[3 + n])
            for n, src in enumerate((low_q, low_k, low_v))
        ]

    for n, (src, start, wide) in enumerate(zip((high_q, high_k, high_v), starts, widths)):
        fetch.append(
            pltpu.make_async_copy(src, high.at[pl.ds(n * rank, rank), pl.ds(start, wide)], in_sem.at[6 + n])
        )
    for n, src in enumerate((norm_a, norm_b)):
        fetch.append(pltpu.make_async_copy(src, norm_in.at[n], in_sem.at[9 + n]))
    for copy in fetch:
        copy.start()

    @pl.when(lead)
    def _():
        for copy in fetch_low(extra.at[my, me]):
            copy.start()

    @pl.when(rest)
    def _():
        for copy in fetch_low(mine):
            copy.start()

    barrier = pltpu.get_barrier_semaphore()

    def tell(other):
        pl.semaphore_signal(barrier, inc=1, device_id=other, device_id_type=MESH)

    @pl.when(first_core != count - 2)
    def _():
        tell({"shard": lax.rem(first_core + 2, count) + 1})

    @pl.when(first_core == 0)
    def _():
        tell({"shard": count - 1})


    @pl.when(lead)
    def _():
        tell({"shard": partner})
        for step in range(1, models):
            tell({"model": lax.rem(my + step, models)})

    def say(which, other):
        pl.semaphore_signal(ready.at[which], inc=1, device_id={"shard": other}, device_id_type=MESH)

    @pl.when(rest & (first_core == 0))
    def _():
        pl.semaphore_wait(barrier, 1)

    @pl.when(rest & (first_core != 0) & (first_core != count - 2))
    def _():
        pl.semaphore_wait(barrier, 3)

    @pl.when(rest & (first_core == count - 2))
    def _():
        pl.semaphore_wait(barrier, 5)
        for other in range(2):
            say(1, other)
        say(0, partner)
        pl.semaphore_signal(ready.at[0], inc=1)

    @pl.when(rest & (first_core != 0))
    def _():
        for other in range(2):
            say(0, lax.rem(first_core + count - 2, count) + other)
        say(1, partner)
        pl.semaphore_signal(ready.at[1], inc=1)

    for copy in fetch[:3]:
        copy.wait()
    pl.semaphore_wait(ready.at[0], 1)

    def block(chip):
        return extra.at[my, pl.ds(chip, 2)]

    def span(p, first=0, rows=deep):
        return raw.at[p, pl.ds(first, rows)]

    def send(ref, sends, recvs, index, to):
        return pltpu.make_async_remote_copy(
            src_ref=ref, dst_ref=ref, send_sem=sends.at[index], recv_sem=recvs.at[index],
            device_id=to, device_id_type=MESH,
        )

    def hop(way, j, ref):
        return send(ref, ring_send, ring_recv, (way, j), {"shard": (right, left)[way]})

    def hand(way, j, ref):
        return send(ref, pair_send, pair_recv, (way, j), {"shard": partner})

    def pass_on(way, kk, chip):
        return send(block(chip), e_send, e_recv, (way, kk), {"shard": (right, left)[way]})

    def across(slot, chip):
        return [
            send(block(chip), y_send, y_recv, (slot, step - 1), {"model": lax.rem(my + step, models)})
            for step in range(1, models)
        ]

    def give(slot, chip):
        return send(extra.at[:, pl.ds(chip, 2)], give_send, give_recv, (slot,), {"shard": partner})

    def give_own(p):
        return pltpu.make_async_remote_copy(
            src_ref=mine, dst_ref=extra.at[my, p],
            send_sem=give_send.at[2 * hops], recv_sem=give_recv.at[2 * hops],
            device_id={"shard": partner}, device_id_type=MESH,
        )

    def chip_of(way, kk):
        far = 2 * (kk + 1)
        return lax.rem(first_core + count + (2 * way - 1) * far, count)

    def slot_of(way, kk):
        return 1 + kk + hops * way

    def moved(j, ref):
        return pltpu.make_async_remote_copy(
            src_ref=ref, dst_ref=ref,
            send_sem=ring_send.at[1, LAST + len(ROWS) + j - MOVED], recv_sem=ring_recv.at[0, LAST + j],
            device_id={"shard": left}, device_id_type=MESH,
        )

    def ways(kk):
        return range(2 if kk < hops - 1 else 1)

    @pl.when(rest)
    def _():
        hop(0, 0, span(me)).start()

    hand(2, 0, raw.at[me]).start()

    @pl.when(rest & (first_core != 0))
    def _():
        pl.semaphore_wait(ready.at[1], 1)
        hop(1, 0, span(me, 0, half)).start()

    for copy in fetch[6:]:
        copy.wait()
    total = norm_in[0] + norm_in[1]
    spread = jnp.concatenate([total, jnp.zeros((1, 128 - total.shape[1]), F32)], axis=1)
    tile = jnp.broadcast_to(spread, (8, 128)).astype(BF16)

    @pl.when(lead)
    def _():
        extra[my, me, 3] = tile

    @pl.when(rest)
    def _():
        mine[3] = tile

    for n in range(3):
        for m in range(3):
            if n != m:
                high[n * rank : (n + 1) * rank, starts[m] : starts[m] + widths[m]] = jnp.zeros(
                    (rank, widths[m]), BF16
                )
    peak[...] = jnp.zeros_like(peak)
    for copy in fetch[3:6]:
        copy.wait()

    @pl.when(lead)
    def _():
        for copy in fetch_low(extra.at[my, me]):
            copy.wait()

    @pl.when(rest)
    def _():
        for copy in fetch_low(mine):
            copy.wait()

    @pl.when(rest)
    def _():
        give_own(me).start()

    @pl.when(rest & (first_core == 0))
    def _():
        pl.semaphore_wait(ready.at[1], 1)
        hop(1, 0, span(me, 0, half)).start()

    @pl.when(rest)
    def _():
        hand(2, 0, raw.at[partner]).wait_recv()
        for way in range(2):
            hop(way, 1, span(partner)).start()
        hop(1, 2, span(me, half, half)).start()

    @pl.when(lead)
    def _():
        give_own(partner).wait_recv()
        pass_on(0, 0, first_core).start()
        pl.semaphore_wait(ready.at[1], 1)
        pass_on(1, 0, first_core).start()
        slots = [(0, first_core)]
        for kk in range(hops):
            for way in ways(kk):
                chip = chip_of(way, kk)
                pass_on(way, kk, chip).wait_recv()
                if kk + 1 < hops and way in ways(kk + 1):
                    pass_on(way, kk + 1, chip).start()
                slots.append((slot_of(way, kk), chip))
        pl.semaphore_wait(barrier, models - 1)
        for slot, chip in slots:
            for copy in across(slot, chip):
                copy.start()
        for slot, chip in slots:
            for copy in across(slot, chip):
                copy.wait_recv()
            give(slot, chip).start()

    def unfold(slot, p, h):
        parts = [
            extra[quarter + h, p, n].astype(F32)
            for n in range(3)
            for quarter in range(0, models, 2)
        ]
        low_n[slot] = jnp.transpose(jnp.concatenate(parts, axis=0), (1, 0)).astype(BF16)

    def merge(p, first, rows, formed=False):
        at = pl.ds(pl.multiple_of(first, 16), rows)
        wide = 256
        for c in range(0, width, wide):
            cols = slice(c, c + wide)
            add = (
                whole[p, at, cols]
                if formed
                else jnp.dot(low_n[0], high[:, cols], preferred_element_type=F32)
            )
            new = raw[p, at, cols].astype(F32) + add
            whole[p, at, cols] = new
            peak[:, cols] = jnp.maximum(
                peak[:, cols], jnp.max(jnp.abs(new).reshape(rows // 8, 8, wide), axis=0)
            )

    def merge_some(number, which):
        @pl.loop(0, number)
        def _(n):
            p, h = which(n)
            unfold(0, p, h)
            merge(p, h * half, half)

    def given(slots):
        @pl.when(rest)
        def _():
            for slot in slots:
                give(slot, first_core).wait_recv()

    PARTS = (
        ((0, 1, 0, deep), (1, 1, 0, half)),
        ((1, 0, 0, deep),),
        ((0, 0, 0, deep), (1, 1, half, half)),
    )
    INDEX = (((0, 2, 0), (1, 3, 0)), ((1, 3, 1),), ((0, 2, 1), (1, 3, 2)))

    def merge_part(kk, part):
        chips = chip_of(0, kk), chip_of(1, kk)

        def way_chip(way):
            return chips[0] + way * (chips[1] - chips[0])

        if part == 0:
            given([slot_of(way, kk) for way in range(2)])
            merge_some(3, lambda n: (way_chip(lax.div(n, 2)) + 1, lax.rem(n, 2)))
        elif part == 1:
            merge_some(2, lambda n: (chips[1], n))
        else:
            merge_some(3, lambda n: (way_chip(lax.div(n, 2)) + lax.div(n, 2), lax.div(n + 1, 2)))

    def merge_own():
        given([0])

        @pl.when(lead)
        def _():
            hand(2, 0, raw.at[partner]).wait_recv()

        merge_some(4, lambda n: (first_core + lax.div(n, 2), lax.rem(n, 2)))

    far = chip_of(0, hops - 1)

    def far_products():
        given([slot_of(0, hops - 1)])

        @pl.loop(0, 4)
        def _(n):
            p, h = far + lax.div(n, 2), lax.rem(n, 2)
            unfold(0, p, h)
            at = pl.ds(pl.multiple_of(h * half, half), half)
            for c in range(0, width, 256):
                whole[p, at, c : c + 256] = jnp.dot(low_n[0], high[:, c : c + 256], preferred_element_type=F32)

    todo = [merge_own]
    events = [(kk, part) for kk in range(hops - 1) for part in range(3)]
    for e, (kk, part) in enumerate(events):
        last = kk == hops - 2

        @pl.when(rest)
        def _():
            for (way, piece, first, rows), (_, per_chip, place) in zip(PARTS[part], INDEX[part]):
                p, n = chip_of(way, kk) + piece, per_chip * kk + place
                hop(way, n, span(p, first, rows)).wait_recv()
                if not last:
                    hop(way, n + per_chip, span(p, first, rows)).start()
                elif piece != way:
                    for j, rows_j in enumerate(ROWS):
                        if way == 0 and j >= MOVED:

                            @pl.when(first_core != count - 2)
                            def _():
                                hop(way, LAST + j, span(p, *rows_j)).start()

                        else:
                            hop(way, LAST + j, span(p, *rows_j)).start()
                elif way == 1 and part == 2:

                    @pl.when(first_core == 2)
                    def _():
                        for j in range(MOVED, len(ROWS)):
                            moved(j, span(p, *ROWS[j])).start()

                hand(way, n, span(p, first, rows)).start()

        if e >= 2:
            todo.pop(0)()
        if e >= 4 and len(todo) > 1:
            todo.pop(0)()
        if e == len(events) - 2:
            far_products()

        @pl.when(lead)
        def _():
            for (way, piece, first, rows), (_, per_chip, place) in zip(PARTS[part], INDEX[part]):
                hand(way, per_chip * kk + place, span(chip_of(way, kk) + piece, first, rows)).wait_recv()

        todo.append(functools.partial(merge_part, kk, part))
    for task in todo:
        task()

    @pl.loop(0, count)
    def _(p):
        norms[:, p] = extra[:, p, 3]

    def sent(copies):
        for copy in copies:
            copy.wait_send()

    @pl.when(lead)
    def _():
        for slot in range(2 * hops):
            sent(across(slot, first_core) + [give(slot, first_core)])
        for kk in range(hops):
            sent([pass_on(way, kk, first_core) for way in ways(kk)])

    @pl.when(rest)
    def _():
        sent([give_own(me)])
        for kk, part in events:
            for (way, piece, first, rows), (_, per_chip, place) in zip(PARTS[part], INDEX[part]):
                n = per_chip * kk + place
                sent([hand(way, n, span(me, first, rows)), hop(way, n, span(me, first, rows))])

    sent([hand(2, 0, raw.at[me])])
    for j, (first, rows) in enumerate(ROWS):

        @pl.when(rest)
        def _():
            for way in range(2):
                hop(way, LAST + j, span(far + 1 - way, first, rows)).wait_recv()
                hand(way, LAST + j, span(far + 1 - way, first, rows)).start()

        @pl.when(lead)
        def _():
            for way in range(2):
                hand(way, LAST + j, span(far + 1 - way, first, rows)).wait_recv()

        for way in range(2):
            merge(far + 1 - way, first, rows, True)
    most[...] = peak[...]

    @pl.when(rest)
    def _():
        for way in range(2):
            for j, (first, rows) in enumerate(ROWS):
                sent([hand(way, LAST + j, span(me, first, rows))])
                if way == 1 or j < MOVED:
                    sent([hop(way, LAST + j, span(me, first, rows))])

    @pl.when(rest & (first_core != count - 2))
    def _():
        sent([hop(0, LAST + j, span(me, *ROWS[j])) for j in range(MOVED, len(ROWS))])

    @pl.when(rest & (first_core == 2))
    def _():
        sent([moved(j, span(me, *ROWS[j])) for j in range(MOVED, len(ROWS))])


def serve_kernel(
    whole, most, norms,
    q, k, v, scale_q, scale_k, scale_v, norm,
    q_out, k_out, v_out, scale_out, per, norm_f, norm_out,
    big_sem, sem,
):
    pieces, deep, width = whole.shape
    outs, stages = (q, k, v), (q_out, k_out, v_out)
    widths = tuple(a.shape[1] for a in outs)
    starts = (0, widths[0], widths[0] + widths[1])
    scale_out[...] = jnp.max(most[...], axis=0, keepdims=True)
    small = []
    for n, (dst, start, wide) in enumerate(zip((scale_q, scale_k, scale_v), starts, widths)):
        small.append(pltpu.make_async_copy(scale_out.at[:, pl.ds(start, wide)], dst, sem.at[n]))
    per[...] = 1.0 / scale_out[...]
    rows = 32

    ends = [sum(BLOCKS[:b]) for b in range(len(BLOCKS) + 1)]

    def out(n, b):
        at = pl.ds(ends[b] * deep, BLOCKS[b] * deep)
        return pltpu.make_async_copy(stages[n].at[at], outs[n].at[at], big_sem.at[n, b])

    for b in range(len(BLOCKS)):

        @pl.loop(ends[b], ends[b + 1])
        def _(p):
            @pl.loop(0, deep // rows)
            def _(r):
                here = pl.ds(pl.multiple_of(r * rows, rows), rows)
                there = pl.ds(pl.multiple_of(p * deep + r * rows, rows), rows)
                for n in range(3):
                    cols = slice(starts[n], starts[n] + widths[n])
                    stages[n][there, :] = (whole[p, here, cols] * per[:, cols]).astype(BF16)

        for n in range(3):
            out(n, b).start()

    models = norms.shape[0]
    wide = norm_f.shape[1] // 2
    for m in range(0, models, 2):
        pair = jnp.concatenate(
            [norms[n].astype(F32)[:, 0, :wide] for n in (m, m + 1)], axis=1
        )
        norm_f[pl.ds(m // 2, pieces, stride=models // 2), :] = pair
    norm_out[...] = norm_f[...].astype(BF16)
    small.append(pltpu.make_async_copy(norm_out, norm, sem.at[3]))
    for copy in small:
        copy.start()
    for copy in small:
        copy.wait()

    for b in range(len(BLOCKS)):
        for n in range(3):
            out(n, b).wait()


def local(count, models, q, low_q, high_q, k, low_k, high_k, v, low_v, high_v, norm_train, norm_step):
    deep, rank = low_q.shape
    widths = (q.shape[1], k.shape[1], v.shape[1])
    width = sum(widths)
    copies = 3 * (count // 4 - 1) + len(ROWS)
    piece = norm_train.shape[0]
    dma = pltpu.SemaphoreType.DMA
    anywhere = pl.BlockSpec(memory_space=pl.ANY)
    vmem = pl.BlockSpec(memory_space=pltpu.VMEM)
    whole, most, norms = pl.pallas_call(
        functools.partial(gather_kernel, count, models),
        out_shape=(
            pltpu.VMEM((count, deep, width), F32),
            pltpu.VMEM((8, width), F32),
            pltpu.VMEM((models, count, 8, 128), BF16),
        ),
        in_specs=[anywhere] * 11,
        out_specs=(vmem, vmem, vmem),
        scratch_shapes=[
            pltpu.VMEM((count, deep, width), BF16),
            pltpu.VMEM((models, count, 4, 8, 128), BF16),
            pltpu.VMEM((4, 8, 128), BF16),
            pltpu.VMEM((1, deep // 2, 3 * rank), BF16),
            pltpu.VMEM((3 * rank, width), BF16),
            pltpu.VMEM((2, 1, piece), F32),
            pltpu.VMEM((8, width), F32),
            dma((11,)),
            dma((count // 2, models - 1)),
            dma((count // 2, models - 1)),
            dma((2, count // 4)),
            dma((2, count // 4)),
            dma((count // 2 + 1,)),
            dma((count // 2 + 1,)),
            dma((2, copies + len(ROWS) - MOVED)),
            dma((2, copies)),
            dma((3, copies)),
            dma((3, copies)),
            pltpu.SemaphoreType.REGULAR((2,)),
        ],
        compiler_params=pltpu.CompilerParams(
            collective_id=0, has_side_effects=True, vmem_limit_bytes=20 * 2**20
        ),
        name="gather",
    )(
        *(
            pltpu.with_memory_space_constraint(a, pltpu.HBM)
            for a in (
                q, k, v, low_q.T, low_k.T, low_v.T, high_q, high_k, high_v,
                norm_train.reshape(1, piece), norm_step.reshape(1, piece),
            )
        )
    )
    total = count * deep
    sizes = tuple((total, w) for w in widths)
    serving_q, serving_k, serving_v, scale_q, scale_k, scale_v, norm = pl.pallas_call(
        serve_kernel,
        out_shape=tuple(jax.ShapeDtypeStruct(s, BF16) for s in sizes)
        + tuple(jax.ShapeDtypeStruct((1, w), F32) for w in widths)
        + (jax.ShapeDtypeStruct((count * models // 2, 2 * piece), BF16),),
        in_specs=[vmem] * 3,
        out_specs=(anywhere,) * 7,
        scratch_shapes=[pltpu.VMEM(s, BF16) for s in sizes]
        + [
            pltpu.VMEM((1, width), F32),
            pltpu.VMEM((1, width), F32),
            pltpu.VMEM((count * models // 2, 2 * piece), F32),
            pltpu.VMEM((count * models // 2, 2 * piece), BF16),
            dma((3, len(BLOCKS))),
            dma((4,)),
        ],
        compiler_params=pltpu.CompilerParams(vmem_limit_bytes=20 * 2**20),
        name="serve",
    )(*(pltpu.with_memory_space_constraint(a, pltpu.VMEM) for a in (whole, most, norms)))
    return (
        serving_q, serving_k, serving_v,
        scale_q.reshape(-1), scale_k.reshape(-1), scale_v.reshape(-1), norm.reshape(-1),
    )


def solution(mesh):
    in_specs = (
        P(("unit", "shard"), "model"),
        P(("unit", "shard"), None),
        P("unit", "model"),
        P(("unit", "shard"), "model"),
        P(("unit", "shard"), None),
        P("unit", "model"),
        P(("unit", "shard"), "model"),
        P(("unit", "shard"), None),
        P("unit", "model"),
        P(("unit", "shard", "model")),
        P(("unit", "shard", "model")),
    )
    out_specs = (
        P("unit", "model"),
        P("unit", "model"),
        P("unit", "model"),
        P(("unit", "model")),
        P(("unit", "model")),
        P(("unit", "model")),
        P("unit"),
    )
    body = functools.partial(local, mesh.shape["shard"], mesh.shape["model"])
    return jax.shard_map(body, mesh=mesh, in_specs=in_specs, out_specs=out_specs, check_vma=False)
```

```python
import functools

import jax
import jax.numpy as jnp
from jax import lax
from jax.experimental import pallas as pl
from jax.experimental.pallas import tpu as pltpu
from jax.sharding import PartitionSpec as P

MESH = pl.DeviceIdType.MESH
F32, BF16 = jnp.float32, jnp.bfloat16
ROWS = ((0, 128), (128, 80), (208, 16), (224, 32))
MOVED = 2
BLOCKS = (1, 1, 2, 4, 4, 4)


def gather_kernel(
    count, models,
    q, k, v, low_q, low_k, low_v, high_q, high_k, high_v, norm_a, norm_b,
    whole, most, norms,
    raw, extra, mine, low_n, high, norm_in, peak,
    in_sem, y_send, y_recv, e_send, e_recv, give_send, give_recv,
    ring_send, ring_recv, pair_send, pair_recv, ready,
):
    me, my = lax.axis_index("shard"), lax.axis_index("model")
    right, left = lax.rem(me + 2, count), lax.rem(me + count - 2, count)
    core = lax.rem(me, 2)
    first_core = me - core
    partner = me + 1 - 2 * core
    over = partner - me
    lead, rest = core == 0, core == 1
    rank = low_q.shape[0]
    half = raw.shape[1] // 2
    hops = count // 4
    deep = raw.shape[1]
    LAST = 3 * (hops - 1)
    widths = (q.shape[1], k.shape[1], v.shape[1])
    starts = (0, widths[0], widths[0] + widths[1])
    width = sum(widths)

    barrier = pltpu.get_barrier_semaphore()

    def tell(other):
        pl.semaphore_signal(barrier, inc=1, device_id=other, device_id_type=MESH)

    @pl.when(first_core != count - 2)
    def _():
        tell({"shard": lax.rem(first_core + 2, count) + 1})

    @pl.when(first_core == 0)
    def _():
        tell({"shard": count - 1})


    @pl.when(lead)
    def _():
        tell({"shard": partner})
        for step in range(1, models):
            tell({"model": lax.rem(my + step, models)})

    fetch = []
    for n, (src, start, wide) in enumerate(zip((q, k, v), starts, widths)):
        fetch.append(pltpu.make_async_copy(src, raw.at[me, :, pl.ds(start, wide)], in_sem.at[n]))
    at = (
        pl.ds(pl.multiple_of(lax.div(my, 2) * 8, 8), 8),
        pl.ds(pl.multiple_of(lax.rem(my, 2) * half, half), half),
    )

    def fetch_low(block):
        return [
            pltpu.make_async_copy(src.at[at], block.at[n], in_sem.at[3 + n])
            for n, src in enumerate((low_q, low_k, low_v))
        ]

    for n, (src, start, wide) in enumerate(zip((high_q, high_k, high_v), starts, widths)):
        fetch.append(
            pltpu.make_async_copy(src, high.at[pl.ds(n * rank, rank), pl.ds(start, wide)], in_sem.at[6 + n])
        )
    for n, src in enumerate((norm_a, norm_b)):
        fetch.append(pltpu.make_async_copy(src, norm_in.at[n], in_sem.at[9 + n]))
    for copy in fetch:
        copy.start()

    @pl.when(lead)
    def _():
        for copy in fetch_low(extra.at[my, me]):
            copy.start()

    @pl.when(rest)
    def _():
        for copy in fetch_low(mine):
            copy.start()

    def say(which, other):
        pl.semaphore_signal(ready.at[which], inc=1, device_id={"shard": other}, device_id_type=MESH)

    @pl.when(rest & (first_core == 0))
    def _():
        pl.semaphore_wait(barrier, 1)

    @pl.when(rest & (first_core != 0) & (first_core != count - 2))
    def _():
        pl.semaphore_wait(barrier, 3)

    @pl.when(rest & (first_core == count - 2))
    def _():
        pl.semaphore_wait(barrier, 5)
        for other in range(2):
            say(1, other)
        say(0, partner)
        pl.semaphore_signal(ready.at[0], inc=1)

    @pl.when(rest & (first_core != 0))
    def _():
        for other in range(2):
            say(0, lax.rem(first_core + count - 2, count) + other)
        say(1, partner)
        pl.semaphore_signal(ready.at[1], inc=1)

    for copy in fetch[:3]:
        copy.wait()
    pl.semaphore_wait(ready.at[0], 1)

    def block(chip):
        return extra.at[my, pl.ds(chip, 2)]

    def span(p, first=0, rows=deep):
        return raw.at[p, pl.ds(first, rows)]

    def send(ref, sends, recvs, index, to):
        return pltpu.make_async_remote_copy(
            src_ref=ref, dst_ref=ref, send_sem=sends.at[index], recv_sem=recvs.at[index],
            device_id=to, device_id_type=MESH,
        )

    def hop(way, j, ref):
        return send(ref, ring_send, ring_recv, (way, j), {"shard": (right, left)[way]})

    def hand(way, j, ref):
        return send(ref, pair_send, pair_recv, (way, j), {"shard": partner})

    def pass_on(way, kk, chip):
        return send(block(chip), e_send, e_recv, (way, kk), {"shard": (right, left)[way]})

    def across(slot, chip):
        return [
            send(block(chip), y_send, y_recv, (slot, step - 1), {"model": lax.rem(my + step, models)})
            for step in range(1, models)
        ]

    def give(slot, chip):
        return send(extra.at[:, pl.ds(chip, 2)], give_send, give_recv, (slot,), {"shard": partner})

    def give_own(p):
        return pltpu.make_async_remote_copy(
            src_ref=mine, dst_ref=extra.at[my, p],
            send_sem=give_send.at[2 * hops], recv_sem=give_recv.at[2 * hops],
            device_id={"shard": partner}, device_id_type=MESH,
        )

    def chip_of(way, kk):
        far = 2 * (kk + 1)
        return lax.rem(first_core + count + (2 * way - 1) * far, count)

    def slot_of(way, kk):
        return 1 + kk + hops * way

    def moved(j, ref):
        return pltpu.make_async_remote_copy(
            src_ref=ref, dst_ref=ref,
            send_sem=ring_send.at[1, LAST + len(ROWS) + j - MOVED], recv_sem=ring_recv.at[0, LAST + j],
            device_id={"shard": left}, device_id_type=MESH,
        )

    def ways(kk):
        return range(2 if kk < hops - 1 else 1)

    @pl.when(rest)
    def _():
        hop(0, 0, span(me)).start()

    hand(2, 0, raw.at[me]).start()

    @pl.when(rest & (first_core != 0))
    def _():
        pl.semaphore_wait(ready.at[1], 1)
        hop(1, 0, span(me, 0, half)).start()

    for copy in fetch[6:]:
        copy.wait()
    total = norm_in[0] + norm_in[1]
    spread = jnp.concatenate([total, jnp.zeros((1, 128 - total.shape[1]), F32)], axis=1)
    tile = jnp.broadcast_to(spread, (8, 128)).astype(BF16)

    @pl.when(lead)
    def _():
        extra[my, me, 3] = tile

    @pl.when(rest)
    def _():
        mine[3] = tile

    for n in range(3):
        for m in range(3):
            if n != m:
                high[n * rank : (n + 1) * rank, starts[m] : starts[m] + widths[m]] = jnp.zeros(
                    (rank, widths[m]), BF16
                )
    peak[...] = jnp.zeros_like(peak)
    for copy in fetch[3:6]:
        copy.wait()

    @pl.when(lead)
    def _():
        for copy in fetch_low(extra.at[my, me]):
            copy.wait()

    @pl.when(rest)
    def _():
        for copy in fetch_low(mine):
            copy.wait()

    @pl.when(rest)
    def _():
        give_own(me).start()

    @pl.when(rest & (first_core == 0))
    def _():
        pl.semaphore_wait(ready.at[1], 1)
        hop(1, 0, span(me, 0, half)).start()

    @pl.when(rest)
    def _():
        hand(2, 0, raw.at[partner]).wait_recv()
        for way in range(2):
            hop(way, 1, span(partner)).start()
        hop(1, 2, span(me, half, half)).start()

    @pl.when(lead)
    def _():
        give_own(partner).wait_recv()
        pass_on(0, 0, first_core).start()
        pl.semaphore_wait(ready.at[1], 1)
        pass_on(1, 0, first_core).start()
        slots = [(0, first_core)]
        for kk in range(hops):
            for way in ways(kk):
                chip = chip_of(way, kk)
                pass_on(way, kk, chip).wait_recv()
                if kk + 1 < hops and way in ways(kk + 1):
                    pass_on(way, kk + 1, chip).start()
                slots.append((slot_of(way, kk), chip))
        pl.semaphore_wait(barrier, models - 1)
        for slot, chip in slots:
            for copy in across(slot, chip):
                copy.start()
        for slot, chip in slots:
            for copy in across(slot, chip):
                copy.wait_recv()
            give(slot, chip).start()

    def unfold(slot, p, h):
        parts = [
            extra[quarter + h, p, n].astype(F32)
            for n in range(3)
            for quarter in range(0, models, 2)
        ]
        low_n[slot] = jnp.transpose(jnp.concatenate(parts, axis=0), (1, 0)).astype(BF16)

    def merge(p, first, rows, formed=False):
        at = pl.ds(pl.multiple_of(first, 16), rows)
        wide = 256
        for c in range(0, width, wide):
            cols = slice(c, c + wide)
            add = (
                whole[p, at, cols]
                if formed
                else jnp.dot(low_n[0], high[:, cols], preferred_element_type=F32)
            )
            new = raw[p, at, cols].astype(F32) + add
            whole[p, at, cols] = new
            peak[:, cols] = jnp.maximum(
                peak[:, cols], jnp.max(jnp.abs(new).reshape(rows // 8, 8, wide), axis=0)
            )

    def merge_some(number, which):
        @pl.loop(0, number)
        def _(n):
            p, h = which(n)
            unfold(0, p, h)
            merge(p, h * half, half)

    def given(slots):
        @pl.when(rest)
        def _():
            for slot in slots:
                give(slot, first_core).wait_recv()

    PARTS = (
        ((0, 1, 0, deep), (1, 1, 0, half)),
        ((1, 0, 0, deep),),
        ((0, 0, 0, deep), (1, 1, half, half)),
    )
    INDEX = (((0, 2, 0), (1, 3, 0)), ((1, 3, 1),), ((0, 2, 1), (1, 3, 2)))

    def merge_part(kk, part):
        chips = chip_of(0, kk), chip_of(1, kk)

        def way_chip(way):
            return chips[0] + way * (chips[1] - chips[0])

        if part == 0:
            given([slot_of(way, kk) for way in range(2)])
            merge_some(3, lambda n: (way_chip(lax.div(n, 2)) + 1, lax.rem(n, 2)))
        elif part == 1:
            merge_some(2, lambda n: (chips[1], n))
        else:
            merge_some(3, lambda n: (way_chip(lax.div(n, 2)) + lax.div(n, 2), lax.div(n + 1, 2)))

    def merge_own():
        given([0])

        @pl.when(lead)
        def _():
            hand(2, 0, raw.at[partner]).wait_recv()

        merge_some(4, lambda n: (first_core + lax.div(n, 2), lax.rem(n, 2)))

    far = chip_of(0, hops - 1)

    def far_products():
        given([slot_of(0, hops - 1)])

        @pl.loop(0, 4)
        def _(n):
            p, h = far + lax.div(n, 2), lax.rem(n, 2)
            unfold(0, p, h)
            at = pl.ds(pl.multiple_of(h * half, half), half)
            for c in range(0, width, 256):
                whole[p, at, c : c + 256] = jnp.dot(low_n[0], high[:, c : c + 256], preferred_element_type=F32)

    todo = [merge_own]
    events = [(kk, part) for kk in range(hops - 1) for part in range(3)]
    for e, (kk, part) in enumerate(events):
        last = kk == hops - 2

        @pl.when(rest)
        def _():
            for (way, piece, first, rows), (_, per_chip, place) in zip(PARTS[part], INDEX[part]):
                p, n = chip_of(way, kk) + piece, per_chip * kk + place
                hop(way, n, span(p, first, rows)).wait_recv()
                if not last:
                    hop(way, n + per_chip, span(p, first, rows)).start()
                elif piece != way:
                    for j, rows_j in enumerate(ROWS):
                        if way == 0 and j >= MOVED:

                            @pl.when(first_core != count - 2)
                            def _():
                                hop(way, LAST + j, span(p, *rows_j)).start()

                        else:
                            hop(way, LAST + j, span(p, *rows_j)).start()
                elif way == 1 and part == 2:

                    @pl.when(first_core == 2)
                    def _():
                        for j in range(MOVED, len(ROWS)):
                            moved(j, span(p, *ROWS[j])).start()

                hand(way, n, span(p, first, rows)).start()

        if e >= 2:
            todo.pop(0)()
        if e >= 4 and len(todo) > 1:
            todo.pop(0)()
        if e == len(events) - 2:
            far_products()

        @pl.when(lead)
        def _():
            for (way, piece, first, rows), (_, per_chip, place) in zip(PARTS[part], INDEX[part]):
                hand(way, per_chip * kk + place, span(chip_of(way, kk) + piece, first, rows)).wait_recv()

        todo.append(functools.partial(merge_part, kk, part))
    for task in todo:
        task()

    @pl.loop(0, count)
    def _(p):
        norms[:, p] = extra[:, p, 3]

    def sent(copies):
        for copy in copies:
            copy.wait_send()

    @pl.when(lead)
    def _():
        for slot in range(2 * hops):
            sent(across(slot, first_core) + [give(slot, first_core)])
        for kk in range(hops):
            sent([pass_on(way, kk, first_core) for way in ways(kk)])

    @pl.when(rest)
    def _():
        sent([give_own(me)])
        for kk, part in events:
            for (way, piece, first, rows), (_, per_chip, place) in zip(PARTS[part], INDEX[part]):
                n = per_chip * kk + place
                sent([hand(way, n, span(me, first, rows)), hop(way, n, span(me, first, rows))])

    sent([hand(2, 0, raw.at[me])])
    for j, (first, rows) in enumerate(ROWS):

        @pl.when(rest)
        def _():
            for way in range(2):
                hop(way, LAST + j, span(far + 1 - way, first, rows)).wait_recv()
                hand(way, LAST + j, span(far + 1 - way, first, rows)).start()

        @pl.when(lead)
        def _():
            for way in range(2):
                hand(way, LAST + j, span(far + 1 - way, first, rows)).wait_recv()

        for way in range(2):
            merge(far + 1 - way, first, rows, True)
    most[...] = peak[...]

    @pl.when(rest)
    def _():
        for way in range(2):
            for j, (first, rows) in enumerate(ROWS):
                sent([hand(way, LAST + j, span(me, first, rows))])
                if way == 1 or j < MOVED:
                    sent([hop(way, LAST + j, span(me, first, rows))])

    @pl.when(rest & (first_core != count - 2))
    def _():
        sent([hop(0, LAST + j, span(me, *ROWS[j])) for j in range(MOVED, len(ROWS))])

    @pl.when(rest & (first_core == 2))
    def _():
        sent([moved(j, span(me, *ROWS[j])) for j in range(MOVED, len(ROWS))])


def serve_kernel(
    whole, most, norms,
    q, k, v, scale_q, scale_k, scale_v, norm,
    q_out, k_out, v_out, scale_out, per, norm_f, norm_out,
    big_sem, sem,
):
    pieces, deep, width = whole.shape
    outs, stages = (q, k, v), (q_out, k_out, v_out)
    widths = tuple(a.shape[1] for a in outs)
    starts = (0, widths[0], widths[0] + widths[1])
    scale_out[...] = jnp.max(most[...], axis=0, keepdims=True)
    small = []
    for n, (dst, start, wide) in enumerate(zip((scale_q, scale_k, scale_v), starts, widths)):
        small.append(pltpu.make_async_copy(scale_out.at[:, pl.ds(start, wide)], dst, sem.at[n]))
    per[...] = 1.0 / scale_out[...]
    rows = 32

    ends = [sum(BLOCKS[:b]) for b in range(len(BLOCKS) + 1)]

    def out(n, b):
        at = pl.ds(ends[b] * deep, BLOCKS[b] * deep)
        return pltpu.make_async_copy(stages[n].at[at], outs[n].at[at], big_sem.at[n, b])

    for b in range(len(BLOCKS)):

        @pl.loop(ends[b], ends[b + 1])
        def _(p):
            @pl.loop(0, deep // rows)
            def _(r):
                here = pl.ds(pl.multiple_of(r * rows, rows), rows)
                there = pl.ds(pl.multiple_of(p * deep + r * rows, rows), rows)
                for n in range(3):
                    cols = slice(starts[n], starts[n] + widths[n])
                    stages[n][there, :] = (whole[p, here, cols] * per[:, cols]).astype(BF16)

        for n in range(3):
            out(n, b).start()

    models = norms.shape[0]
    wide = norm_f.shape[1] // 2
    for m in range(0, models, 2):
        pair = jnp.concatenate(
            [norms[n].astype(F32)[:, 0, :wide] for n in (m, m + 1)], axis=1
        )
        norm_f[pl.ds(m // 2, pieces, stride=models // 2), :] = pair
    norm_out[...] = norm_f[...].astype(BF16)
    small.append(pltpu.make_async_copy(norm_out, norm, sem.at[3]))
    for copy in small:
        copy.start()
    for copy in small:
        copy.wait()

    for b in range(len(BLOCKS)):
        for n in range(3):
            out(n, b).wait()


def local(count, models, q, low_q, high_q, k, low_k, high_k, v, low_v, high_v, norm_train, norm_step):
    deep, rank = low_q.shape
    widths = (q.shape[1], k.shape[1], v.shape[1])
    width = sum(widths)
    copies = 3 * (count // 4 - 1) + len(ROWS)
    piece = norm_train.shape[0]
    dma = pltpu.SemaphoreType.DMA
    anywhere = pl.BlockSpec(memory_space=pl.ANY)
    vmem = pl.BlockSpec(memory_space=pltpu.VMEM)
    whole, most, norms = pl.pallas_call(
        functools.partial(gather_kernel, count, models),
        out_shape=(
            pltpu.VMEM((count, deep, width), F32),
            pltpu.VMEM((8, width), F32),
            pltpu.VMEM((models, count, 8, 128), BF16),
        ),
        in_specs=[anywhere] * 11,
        out_specs=(vmem, vmem, vmem),
        scratch_shapes=[
            pltpu.VMEM((count, deep, width), BF16),
            pltpu.VMEM((models, count, 4, 8, 128), BF16),
            pltpu.VMEM((4, 8, 128), BF16),
            pltpu.VMEM((1, deep // 2, 3 * rank), BF16),
            pltpu.VMEM((3 * rank, width), BF16),
            pltpu.VMEM((2, 1, piece), F32),
            pltpu.VMEM((8, width), F32),
            dma((11,)),
            dma((count // 2, models - 1)),
            dma((count // 2, models - 1)),
            dma((2, count // 4)),
            dma((2, count // 4)),
            dma((count // 2 + 1,)),
            dma((count // 2 + 1,)),
            dma((2, copies + len(ROWS) - MOVED)),
            dma((2, copies)),
            dma((3, copies)),
            dma((3, copies)),
            pltpu.SemaphoreType.REGULAR((2,)),
        ],
        compiler_params=pltpu.CompilerParams(
            collective_id=0, has_side_effects=True, vmem_limit_bytes=20 * 2**20
        ),
        name="gather",
    )(
        *(
            pltpu.with_memory_space_constraint(a, pltpu.HBM)
            for a in (
                q, k, v, low_q.T, low_k.T, low_v.T, high_q, high_k, high_v,
                norm_train.reshape(1, piece), norm_step.reshape(1, piece),
            )
        )
    )
    total = count * deep
    sizes = tuple((total, w) for w in widths)
    serving_q, serving_k, serving_v, scale_q, scale_k, scale_v, norm = pl.pallas_call(
        serve_kernel,
        out_shape=tuple(jax.ShapeDtypeStruct(s, BF16) for s in sizes)
        + tuple(jax.ShapeDtypeStruct((1, w), F32) for w in widths)
        + (jax.ShapeDtypeStruct((count * models // 2, 2 * piece), BF16),),
        in_specs=[vmem] * 3,
        out_specs=(anywhere,) * 7,
        scratch_shapes=[pltpu.VMEM(s, BF16) for s in sizes]
        + [
            pltpu.VMEM((1, width), F32),
            pltpu.VMEM((1, width), F32),
            pltpu.VMEM((count * models // 2, 2 * piece), F32),
            pltpu.VMEM((count * models // 2, 2 * piece), BF16),
            dma((3, len(BLOCKS))),
            dma((4,)),
        ],
        compiler_params=pltpu.CompilerParams(vmem_limit_bytes=20 * 2**20),
        name="serve",
    )(*(pltpu.with_memory_space_constraint(a, pltpu.VMEM) for a in (whole, most, norms)))
    return (
        serving_q, serving_k, serving_v,
        scale_q.reshape(-1), scale_k.reshape(-1), scale_v.reshape(-1), norm.reshape(-1),
    )


def solution(mesh):
    in_specs = (
        P(("unit", "shard"), "model"),
        P(("unit", "shard"), None),
        P("unit", "model"),
        P(("unit", "shard"), "model"),
        P(("unit", "shard"), None),
        P("unit", "model"),
        P(("unit", "shard"), "model"),
        P(("unit", "shard"), None),
        P("unit", "model"),
        P(("unit", "shard", "model")),
        P(("unit", "shard", "model")),
    )
    out_specs = (
        P("unit", "model"),
        P("unit", "model"),
        P("unit", "model"),
        P(("unit", "model")),
        P(("unit", "model")),
        P(("unit", "model")),
        P("unit"),
    )
    body = functools.partial(local, mesh.shape["shard"], mesh.shape["model"])
    return jax.shard_map(body, mesh=mesh, in_specs=in_specs, out_specs=out_specs, check_vma=False)
```

```python
import functools

import jax
import jax.numpy as jnp
from jax import lax
from jax.experimental import pallas as pl
from jax.experimental.pallas import tpu as pltpu
from jax.sharding import PartitionSpec as P

MESH = pl.DeviceIdType.MESH
F32, BF16 = jnp.float32, jnp.bfloat16
ROWS = ((0, 128), (128, 80), (208, 16), (224, 16), (240, 16))
MOVED = 2
BLOCKS = (1, 2, 4, 9)


def gather_kernel(
    count, models,
    q, k, v, low_q, low_k, low_v, high_q, high_k, high_v, norm_a, norm_b,
    whole, most, norms,
    raw, extra, mine, low_n, high, norm_in, peak,
    in_sem, y_send, y_recv, e_send, e_recv, give_send, give_recv,
    ring_send, ring_recv, pair_send, pair_recv, ready,
):
    me, my = lax.axis_index("shard"), lax.axis_index("model")
    right, left = lax.rem(me + 2, count), lax.rem(me + count - 2, count)
    core = lax.rem(me, 2)
    first_core = me - core
    partner = me + 1 - 2 * core
    over = partner - me
    lead, rest = core == 0, core == 1
    rank = low_q.shape[0]
    half = raw.shape[1] // 2
    hops = count // 4
    deep = raw.shape[1]
    LAST = 3 * (hops - 1)
    widths = (q.shape[1], k.shape[1], v.shape[1])
    starts = (0, widths[0], widths[0] + widths[1])
    width = sum(widths)

    barrier = pltpu.get_barrier_semaphore()

    def tell(other):
        pl.semaphore_signal(barrier, inc=1, device_id=other, device_id_type=MESH)

    @pl.when(first_core != count - 2)
    def _():
        tell({"shard": lax.rem(first_core + 2, count) + 1})

    @pl.when(first_core == 0)
    def _():
        tell({"shard": count - 1})


    @pl.when(lead)
    def _():
        tell({"shard": partner})
        for step in range(1, models):
            tell({"model": lax.rem(my + step, models)})

    fetch = []
    for n, (src, start, wide) in enumerate(zip((q, k, v), starts, widths)):
        fetch.append(pltpu.make_async_copy(src, raw.at[me, :, pl.ds(start, wide)], in_sem.at[n]))
    at = (
        pl.ds(pl.multiple_of(lax.div(my, 2) * 8, 8), 8),
        pl.ds(pl.multiple_of(lax.rem(my, 2) * half, half), half),
    )

    def fetch_low(block):
        return [
            pltpu.make_async_copy(src.at[at], block.at[n], in_sem.at[3 + n])
            for n, src in enumerate((low_q, low_k, low_v))
        ]

    for n, (src, start, wide) in enumerate(zip((high_q, high_k, high_v), starts, widths)):
        fetch.append(
            pltpu.make_async_copy(src, high.at[pl.ds(n * rank, rank), pl.ds(start, wide)], in_sem.at[6 + n])
        )
    for n, src in enumerate((norm_a, norm_b)):
        fetch.append(pltpu.make_async_copy(src, norm_in.at[n], in_sem.at[9 + n]))
    for copy in fetch:
        copy.start()

    @pl.when(lead)
    def _():
        for copy in fetch_low(extra.at[my, me]):
            copy.start()

    @pl.when(rest)
    def _():
        for copy in fetch_low(mine):
            copy.start()

    def say(which, other):
        pl.semaphore_signal(ready.at[which], inc=1, device_id={"shard": other}, device_id_type=MESH)

    @pl.when(rest & (first_core == 0))
    def _():
        pl.semaphore_wait(barrier, 1)

    @pl.when(rest & (first_core != 0) & (first_core != count - 2))
    def _():
        pl.semaphore_wait(barrier, 3)

    @pl.when(rest & (first_core == count - 2))
    def _():
        pl.semaphore_wait(barrier, 5)
        for other in range(2):
            say(1, other)
        say(0, partner)
        pl.semaphore_signal(ready.at[0], inc=1)

    @pl.when(rest & (first_core != 0))
    def _():
        for other in range(2):
            say(0, lax.rem(first_core + count - 2, count) + other)
        say(1, partner)
        pl.semaphore_signal(ready.at[1], inc=1)

    for copy in fetch[:3]:
        copy.wait()
    pl.semaphore_wait(ready.at[0], 1)

    def block(chip):
        return extra.at[my, pl.ds(chip, 2)]

    def span(p, first=0, rows=deep):
        return raw.at[p, pl.ds(first, rows)]

    def send(ref, sends, recvs, index, to):
        return pltpu.make_async_remote_copy(
            src_ref=ref, dst_ref=ref, send_sem=sends.at[index], recv_sem=recvs.at[index],
            device_id=to, device_id_type=MESH,
        )

    def hop(way, j, ref):
        return send(ref, ring_send, ring_recv, (way, j), {"shard": (right, left)[way]})

    def hand(way, j, ref):
        return send(ref, pair_send, pair_recv, (way, j), {"shard": partner})

    def pass_on(way, kk, chip):
        return send(block(chip), e_send, e_recv, (way, kk), {"shard": (right, left)[way]})

    def across(slot, chip):
        return [
            send(block(chip), y_send, y_recv, (slot, step - 1), {"model": lax.rem(my + step, models)})
            for step in range(1, models)
        ]

    def give(slot, chip):
        return send(extra.at[:, pl.ds(chip, 2)], give_send, give_recv, (slot,), {"shard": partner})

    def give_own(p):
        return pltpu.make_async_remote_copy(
            src_ref=mine, dst_ref=extra.at[my, p],
            send_sem=give_send.at[2 * hops], recv_sem=give_recv.at[2 * hops],
            device_id={"shard": partner}, device_id_type=MESH,
        )

    def chip_of(way, kk):
        far = 2 * (kk + 1)
        return lax.rem(first_core + count + (2 * way - 1) * far, count)

    def slot_of(way, kk):
        return 1 + kk + hops * way

    def moved(j, ref):
        return pltpu.make_async_remote_copy(
            src_ref=ref, dst_ref=ref,
            send_sem=ring_send.at[1, LAST + len(ROWS) + j - MOVED], recv_sem=ring_recv.at[0, LAST + j],
            device_id={"shard": left}, device_id_type=MESH,
        )

    def ways(kk):
        return range(2 if kk < hops - 1 else 1)

    @pl.when(rest)
    def _():
        hop(0, 0, span(me)).start()

    hand(2, 0, raw.at[me]).start()

    @pl.when(rest & (first_core != 0))
    def _():
        pl.semaphore_wait(ready.at[1], 1)
        hop(1, 0, span(me, 0, half)).start()

    for copy in fetch[6:]:
        copy.wait()
    total = norm_in[0] + norm_in[1]
    spread = jnp.concatenate([total, jnp.zeros((1, 128 - total.shape[1]), F32)], axis=1)
    tile = jnp.broadcast_to(spread, (8, 128)).astype(BF16)

    @pl.when(lead)
    def _():
        extra[my, me, 3] = tile

    @pl.when(rest)
    def _():
        mine[3] = tile

    for n in range(3):
        for m in range(3):
            if n != m:
                high[n * rank : (n + 1) * rank, starts[m] : starts[m] + widths[m]] = jnp.zeros(
                    (rank, widths[m]), BF16
                )
    peak[...] = jnp.zeros_like(peak)
    for copy in fetch[3:6]:
        copy.wait()

    @pl.when(lead)
    def _():
        for copy in fetch_low(extra.at[my, me]):
            copy.wait()

    @pl.when(rest)
    def _():
        for copy in fetch_low(mine):
            copy.wait()

    @pl.when(rest)
    def _():
        give_own(me).start()

    @pl.when(rest & (first_core == 0))
    def _():
        pl.semaphore_wait(ready.at[1], 1)
        hop(1, 0, span(me, 0, half)).start()

    @pl.when(rest)
    def _():
        hand(2, 0, raw.at[partner]).wait_recv()
        for way in range(2):
            hop(way, 1, span(partner)).start()
        hop(1, 2, span(me, half, half)).start()

    @pl.when(lead)
    def _():
        give_own(partner).wait_recv()
        pass_on(0, 0, first_core).start()
        pl.semaphore_wait(ready.at[1], 1)
        pass_on(1, 0, first_core).start()
        slots = [(0, first_core)]
        for kk in range(hops):
            for way in ways(kk):
                chip = chip_of(way, kk)
                pass_on(way, kk, chip).wait_recv()
                if kk + 1 < hops and way in ways(kk + 1):
                    pass_on(way, kk + 1, chip).start()
                slots.append((slot_of(way, kk), chip))
        pl.semaphore_wait(barrier, models - 1)
        for slot, chip in slots:
            for copy in across(slot, chip):
                copy.start()
        for slot, chip in slots:
            for copy in across(slot, chip):
                copy.wait_recv()
            give(slot, chip).start()

    def unfold(slot, p, h):
        parts = [
            extra[quarter + h, p, n].astype(F32)
            for n in range(3)
            for quarter in range(0, models, 2)
        ]
        low_n[slot] = jnp.transpose(jnp.concatenate(parts, axis=0), (1, 0)).astype(BF16)

    def merge(p, first, rows, formed=False):
        at = pl.ds(pl.multiple_of(first, 16), rows)
        wide = 256
        for c in range(0, width, wide):
            cols = slice(c, c + wide)
            add = (
                whole[p, at, cols]
                if formed
                else jnp.dot(low_n[0], high[:, cols], preferred_element_type=F32)
            )
            new = raw[p, at, cols].astype(F32) + add
            whole[p, at, cols] = new
            peak[:, cols] = jnp.maximum(
                peak[:, cols], jnp.max(jnp.abs(new).reshape(rows // 8, 8, wide), axis=0)
            )

    def merge_some(number, which):
        @pl.loop(0, number)
        def _(n):
            p, h = which(n)
            unfold(0, p, h)
            merge(p, h * half, half)

    def given(slots):
        @pl.when(rest)
        def _():
            for slot in slots:
                give(slot, first_core).wait_recv()

    PARTS = (
        ((0, 1, 0, deep), (1, 1, 0, half)),
        ((1, 0, 0, deep),),
        ((0, 0, 0, deep), (1, 1, half, half)),
    )
    INDEX = (((0, 2, 0), (1, 3, 0)), ((1, 3, 1),), ((0, 2, 1), (1, 3, 2)))

    def merge_part(kk, part):
        chips = chip_of(0, kk), chip_of(1, kk)

        def way_chip(way):
            return chips[0] + way * (chips[1] - chips[0])

        if part == 0:
            given([slot_of(way, kk) for way in range(2)])
            merge_some(3, lambda n: (way_chip(lax.div(n, 2)) + 1, lax.rem(n, 2)))
        elif part == 1:
            merge_some(2, lambda n: (chips[1], n))
        else:
            merge_some(3, lambda n: (way_chip(lax.div(n, 2)) + lax.div(n, 2), lax.div(n + 1, 2)))

    def merge_own():
        given([0])

        @pl.when(lead)
        def _():
            hand(2, 0, raw.at[partner]).wait_recv()

        merge_some(4, lambda n: (first_core + lax.div(n, 2), lax.rem(n, 2)))

    far = chip_of(0, hops - 1)

    def far_products():
        given([slot_of(0, hops - 1)])

        @pl.loop(0, 4)
        def _(n):
            p, h = far + lax.div(n, 2), lax.rem(n, 2)
            unfold(0, p, h)
            at = pl.ds(pl.multiple_of(h * half, half), half)
            for c in range(0, width, 256):
                whole[p, at, c : c + 256] = jnp.dot(low_n[0], high[:, c : c + 256], preferred_element_type=F32)

    todo = [merge_own]
    events = [(kk, part) for kk in range(hops - 1) for part in range(3)]
    for e, (kk, part) in enumerate(events):
        last = kk == hops - 2

        @pl.when(rest)
        def _():
            for (way, piece, first, rows), (_, per_chip, place) in zip(PARTS[part], INDEX[part]):
                p, n = chip_of(way, kk) + piece, per_chip * kk + place
                hop(way, n, span(p, first, rows)).wait_recv()
                if not last:
                    hop(way, n + per_chip, span(p, first, rows)).start()
                elif piece != way:
                    for j, rows_j in enumerate(ROWS):
                        if way == 0 and j >= MOVED:

                            @pl.when(first_core != count - 2)
                            def _():
                                hop(way, LAST + j, span(p, *rows_j)).start()

                        else:
                            hop(way, LAST + j, span(p, *rows_j)).start()
                elif way == 1 and part == 2:

                    @pl.when(first_core == 2)
                    def _():
                        for j in range(MOVED, len(ROWS)):
                            moved(j, span(p, *ROWS[j])).start()

                hand(way, n, span(p, first, rows)).start()

        if e >= 2:
            todo.pop(0)()
        if e >= 4 and len(todo) > 1:
            todo.pop(0)()
        if e == len(events) - 2:
            far_products()

        @pl.when(lead)
        def _():
            for (way, piece, first, rows), (_, per_chip, place) in zip(PARTS[part], INDEX[part]):
                hand(way, per_chip * kk + place, span(chip_of(way, kk) + piece, first, rows)).wait_recv()

        todo.append(functools.partial(merge_part, kk, part))
    for task in todo:
        task()

    @pl.loop(0, count)
    def _(p):
        norms[:, p] = extra[:, p, 3]

    def sent(copies):
        for copy in copies:
            copy.wait_send()

    @pl.when(lead)
    def _():
        for slot in range(2 * hops):
            sent(across(slot, first_core) + [give(slot, first_core)])
        for kk in range(hops):
            sent([pass_on(way, kk, first_core) for way in ways(kk)])

    @pl.when(rest)
    def _():
        sent([give_own(me)])
        for kk, part in events:
            for (way, piece, first, rows), (_, per_chip, place) in zip(PARTS[part], INDEX[part]):
                n = per_chip * kk + place
                sent([hand(way, n, span(me, first, rows)), hop(way, n, span(me, first, rows))])

    sent([hand(2, 0, raw.at[me])])
    for j, (first, rows) in enumerate(ROWS):

        @pl.when(rest)
        def _():
            for way in range(2):
                hop(way, LAST + j, span(far + 1 - way, first, rows)).wait_recv()
                hand(way, LAST + j, span(far + 1 - way, first, rows)).start()

        @pl.when(lead)
        def _():
            for way in range(2):
                hand(way, LAST + j, span(far + 1 - way, first, rows)).wait_recv()

        for way in range(2):
            merge(far + 1 - way, first, rows, True)
    most[...] = peak[...]

    @pl.when(rest)
    def _():
        for way in range(2):
            for j, (first, rows) in enumerate(ROWS):
                sent([hand(way, LAST + j, span(me, first, rows))])
                if way == 1 or j < MOVED:
                    sent([hop(way, LAST + j, span(me, first, rows))])

    @pl.when(rest & (first_core != count - 2))
    def _():
        sent([hop(0, LAST + j, span(me, *ROWS[j])) for j in range(MOVED, len(ROWS))])

    @pl.when(rest & (first_core == 2))
    def _():
        sent([moved(j, span(me, *ROWS[j])) for j in range(MOVED, len(ROWS))])


def serve_kernel(
    whole, most, norms,
    q, k, v, scale_q, scale_k, scale_v, norm,
    q_out, k_out, v_out, scale_out, per, norm_f, norm_out,
    big_sem, sem,
):
    pieces, deep, width = whole.shape
    outs, stages = (q, k, v), (q_out, k_out, v_out)
    widths = tuple(a.shape[1] for a in outs)
    starts = (0, widths[0], widths[0] + widths[1])
    scale_out[...] = jnp.max(most[...], axis=0, keepdims=True)
    small = []
    for n, (dst, start, wide) in enumerate(zip((scale_q, scale_k, scale_v), starts, widths)):
        small.append(pltpu.make_async_copy(scale_out.at[:, pl.ds(start, wide)], dst, sem.at[n]))
    per[...] = 1.0 / scale_out[...]
    rows = 32

    ends = [sum(BLOCKS[:b]) for b in range(len(BLOCKS) + 1)]

    def out(n, b):
        at = pl.ds(ends[b] * deep, BLOCKS[b] * deep)
        return pltpu.make_async_copy(stages[n].at[at], outs[n].at[at], big_sem.at[n, b])

    for b in range(len(BLOCKS)):

        @pl.loop(ends[b], ends[b + 1])
        def _(p):
            @pl.loop(0, deep // rows)
            def _(r):
                here = pl.ds(pl.multiple_of(r * rows, rows), rows)
                there = pl.ds(pl.multiple_of(p * deep + r * rows, rows), rows)
                for n in range(3):
                    cols = slice(starts[n], starts[n] + widths[n])
                    stages[n][there, :] = (whole[p, here, cols] * per[:, cols]).astype(BF16)

        for n in range(3):
            out(n, b).start()

    models = norms.shape[0]
    wide = norm_f.shape[1] // 2
    for m in range(0, models, 2):
        pair = jnp.concatenate(
            [norms[n].astype(F32)[:, 0, :wide] for n in (m, m + 1)], axis=1
        )
        norm_f[pl.ds(m // 2, pieces, stride=models // 2), :] = pair
    norm_out[...] = norm_f[...].astype(BF16)
    small.append(pltpu.make_async_copy(norm_out, norm, sem.at[3]))
    for copy in small:
        copy.start()
    for copy in small:
        copy.wait()

    for b in range(len(BLOCKS)):
        for n in range(3):
            out(n, b).wait()


def local(count, models, q, low_q, high_q, k, low_k, high_k, v, low_v, high_v, norm_train, norm_step):
    deep, rank = low_q.shape
    widths = (q.shape[1], k.shape[1], v.shape[1])
    width = sum(widths)
    copies = 3 * (count // 4 - 1) + len(ROWS)
    piece = norm_train.shape[0]
    dma = pltpu.SemaphoreType.DMA
    anywhere = pl.BlockSpec(memory_space=pl.ANY)
    vmem = pl.BlockSpec(memory_space=pltpu.VMEM)
    whole, most, norms = pl.pallas_call(
        functools.partial(gather_kernel, count, models),
        out_shape=(
            pltpu.VMEM((count, deep, width), F32),
            pltpu.VMEM((8, width), F32),
            pltpu.VMEM((models, count, 8, 128), BF16),
        ),
        in_specs=[anywhere] * 11,
        out_specs=(vmem, vmem, vmem),
        scratch_shapes=[
            pltpu.VMEM((count, deep, width), BF16),
            pltpu.VMEM((models, count, 4, 8, 128), BF16),
            pltpu.VMEM((4, 8, 128), BF16),
            pltpu.VMEM((1, deep // 2, 3 * rank), BF16),
            pltpu.VMEM((3 * rank, width), BF16),
            pltpu.VMEM((2, 1, piece), F32),
            pltpu.VMEM((8, width), F32),
            dma((11,)),
            dma((count // 2, models - 1)),
            dma((count // 2, models - 1)),
            dma((2, count // 4)),
            dma((2, count // 4)),
            dma((count // 2 + 1,)),
            dma((count // 2 + 1,)),
            dma((2, copies + len(ROWS) - MOVED)),
            dma((2, copies)),
            dma((3, copies)),
            dma((3, copies)),
            pltpu.SemaphoreType.REGULAR((2,)),
        ],
        compiler_params=pltpu.CompilerParams(
            collective_id=0, has_side_effects=True, vmem_limit_bytes=20 * 2**20
        ),
        name="gather",
    )(
        *(
            pltpu.with_memory_space_constraint(a, pltpu.HBM)
            for a in (
                q, k, v, low_q.T, low_k.T, low_v.T, high_q, high_k, high_v,
                norm_train.reshape(1, piece), norm_step.reshape(1, piece),
            )
        )
    )
    total = count * deep
    sizes = tuple((total, w) for w in widths)
    serving_q, serving_k, serving_v, scale_q, scale_k, scale_v, norm = pl.pallas_call(
        serve_kernel,
        out_shape=tuple(jax.ShapeDtypeStruct(s, BF16) for s in sizes)
        + tuple(jax.ShapeDtypeStruct((1, w), F32) for w in widths)
        + (jax.ShapeDtypeStruct((count * models // 2, 2 * piece), BF16),),
        in_specs=[vmem] * 3,
        out_specs=(anywhere,) * 7,
        scratch_shapes=[pltpu.VMEM(s, BF16) for s in sizes]
        + [
            pltpu.VMEM((1, width), F32),
            pltpu.VMEM((1, width), F32),
            pltpu.VMEM((count * models // 2, 2 * piece), F32),
            pltpu.VMEM((count * models // 2, 2 * piece), BF16),
            dma((3, len(BLOCKS))),
            dma((4,)),
        ],
        compiler_params=pltpu.CompilerParams(vmem_limit_bytes=20 * 2**20),
        name="serve",
    )(*(pltpu.with_memory_space_constraint(a, pltpu.VMEM) for a in (whole, most, norms)))
    return (
        serving_q, serving_k, serving_v,
        scale_q.reshape(-1), scale_k.reshape(-1), scale_v.reshape(-1), norm.reshape(-1),
    )


def solution(mesh):
    in_specs = (
        P(("unit", "shard"), "model"),
        P(("unit", "shard"), None),
        P("unit", "model"),
        P(("unit", "shard"), "model"),
        P(("unit", "shard"), None),
        P("unit", "model"),
        P(("unit", "shard"), "model"),
        P(("unit", "shard"), None),
        P("unit", "model"),
        P(("unit", "shard", "model")),
        P(("unit", "shard", "model")),
    )
    out_specs = (
        P("unit", "model"),
        P("unit", "model"),
        P("unit", "model"),
        P(("unit", "model")),
        P(("unit", "model")),
        P(("unit", "model")),
        P("unit"),
    )
    body = functools.partial(local, mesh.shape["shard"], mesh.shape["model"])
    return jax.shard_map(body, mesh=mesh, in_specs=in_specs, out_specs=out_specs, check_vma=False)
```

```python
import functools

import jax
import jax.numpy as jnp
from jax import lax
from jax.experimental import pallas as pl
from jax.experimental.pallas import tpu as pltpu
from jax.sharding import PartitionSpec as P

MESH = pl.DeviceIdType.MESH
F32, BF16 = jnp.float32, jnp.bfloat16
ROWS = ((0, 128), (128, 80), (208, 16), (224, 32))
MOVED = 2
BLOCKS = (1, 1, 2, 3, 3, 3, 3)


def gather_kernel(
    count, models,
    q, k, v, low_q, low_k, low_v, high_q, high_k, high_v, norm_a, norm_b,
    whole, most, norms,
    raw, extra, mine, low_n, high, norm_in, peak,
    in_sem, y_send, y_recv, e_send, e_recv, give_send, give_recv,
    ring_send, ring_recv, pair_send, pair_recv, ready,
):
    me, my = lax.axis_index("shard"), lax.axis_index("model")
    right, left = lax.rem(me + 2, count), lax.rem(me + count - 2, count)
    core = lax.rem(me, 2)
    first_core = me - core
    partner = me + 1 - 2 * core
    over = partner - me
    lead, rest = core == 0, core == 1
    rank = low_q.shape[0]
    half = raw.shape[1] // 2
    hops = count // 4
    deep = raw.shape[1]
    LAST = 3 * (hops - 1)
    widths = (q.shape[1], k.shape[1], v.shape[1])
    starts = (0, widths[0], widths[0] + widths[1])
    width = sum(widths)

    barrier = pltpu.get_barrier_semaphore()

    def tell(other):
        pl.semaphore_signal(barrier, inc=1, device_id=other, device_id_type=MESH)

    @pl.when(first_core != count - 2)
    def _():
        tell({"shard": lax.rem(first_core + 2, count) + 1})

    @pl.when(first_core == 0)
    def _():
        tell({"shard": count - 1})


    @pl.when(lead)
    def _():
        tell({"shard": partner})
        for step in range(1, models):
            tell({"model": lax.rem(my + step, models)})

    fetch = []
    for n, (src, start, wide) in enumerate(zip((q, k, v), starts, widths)):
        fetch.append(pltpu.make_async_copy(src, raw.at[me, :, pl.ds(start, wide)], in_sem.at[n]))
    at = (
        pl.ds(pl.multiple_of(lax.div(my, 2) * 8, 8), 8),
        pl.ds(pl.multiple_of(lax.rem(my, 2) * half, half), half),
    )

    def fetch_low(block):
        return [
            pltpu.make_async_copy(src.at[at], block.at[n], in_sem.at[3 + n])
            for n, src in enumerate((low_q, low_k, low_v))
        ]

    for n, (src, start, wide) in enumerate(zip((high_q, high_k, high_v), starts, widths)):
        fetch.append(
            pltpu.make_async_copy(src, high.at[pl.ds(n * rank, rank), pl.ds(start, wide)], in_sem.at[6 + n])
        )
    for n, src in enumerate((norm_a, norm_b)):
        fetch.append(pltpu.make_async_copy(src, norm_in.at[n], in_sem.at[9 + n]))
    for copy in fetch:
        copy.start()

    @pl.when(lead)
    def _():
        for copy in fetch_low(extra.at[my, me]):
            copy.start()

    @pl.when(rest)
    def _():
        for copy in fetch_low(mine):
            copy.start()

    def say(which, other):
        pl.semaphore_signal(ready.at[which], inc=1, device_id={"shard": other}, device_id_type=MESH)

    @pl.when(rest & (first_core == 0))
    def _():
        pl.semaphore_wait(barrier, 1)

    @pl.when(rest & (first_core != 0) & (first_core != count - 2))
    def _():
        pl.semaphore_wait(barrier, 3)

    @pl.when(rest & (first_core == count - 2))
    def _():
        pl.semaphore_wait(barrier, 5)
        for other in range(2):
            say(1, other)
        say(0, partner)
        pl.semaphore_signal(ready.at[0], inc=1)

    @pl.when(rest & (first_core != 0))
    def _():
        for other in range(2):
            say(0, lax.rem(first_core + count - 2, count) + other)
        say(1, partner)
        pl.semaphore_signal(ready.at[1], inc=1)

    for copy in fetch[:3]:
        copy.wait()
    pl.semaphore_wait(ready.at[0], 1)

    def block(chip):
        return extra.at[my, pl.ds(chip, 2)]

    def span(p, first=0, rows=deep):
        return raw.at[p, pl.ds(first, rows)]

    def send(ref, sends, recvs, index, to):
        return pltpu.make_async_remote_copy(
            src_ref=ref, dst_ref=ref, send_sem=sends.at[index], recv_sem=recvs.at[index],
            device_id=to, device_id_type=MESH,
        )

    def hop(way, j, ref):
        return send(ref, ring_send, ring_recv, (way, j), {"shard": (right, left)[way]})

    def hand(way, j, ref):
        return send(ref, pair_send, pair_recv, (way, j), {"shard": partner})

    def pass_on(way, kk, chip):
        return send(block(chip), e_send, e_recv, (way, kk), {"shard": (right, left)[way]})

    def across(slot, chip):
        return [
            send(block(chip), y_send, y_recv, (slot, step - 1), {"model": lax.rem(my + step, models)})
            for step in range(1, models)
        ]

    def give(slot, chip):
        return send(extra.at[:, pl.ds(chip, 2)], give_send, give_recv, (slot,), {"shard": partner})

    def give_own(p):
        return pltpu.make_async_remote_copy(
            src_ref=mine, dst_ref=extra.at[my, p],
            send_sem=give_send.at[2 * hops], recv_sem=give_recv.at[2 * hops],
            device_id={"shard": partner}, device_id_type=MESH,
        )

    def chip_of(way, kk):
        far = 2 * (kk + 1)
        return lax.rem(first_core + count + (2 * way - 1) * far, count)

    def slot_of(way, kk):
        return 1 + kk + hops * way

    def moved(j, ref):
        return pltpu.make_async_remote_copy(
            src_ref=ref, dst_ref=ref,
            send_sem=ring_send.at[1, LAST + len(ROWS) + j - MOVED], recv_sem=ring_recv.at[0, LAST + j],
            device_id={"shard": left}, device_id_type=MESH,
        )

    def ways(kk):
        return range(2 if kk < hops - 1 else 1)

    @pl.when(rest)
    def _():
        hop(0, 0, span(me)).start()

    hand(2, 0, raw.at[me]).start()

    @pl.when(rest & (first_core != 0))
    def _():
        pl.semaphore_wait(ready.at[1], 1)
        hop(1, 0, span(me, 0, half)).start()

    for copy in fetch[6:]:
        copy.wait()
    total = norm_in[0] + norm_in[1]
    spread = jnp.concatenate([total, jnp.zeros((1, 128 - total.shape[1]), F32)], axis=1)
    tile = jnp.broadcast_to(spread, (8, 128)).astype(BF16)

    @pl.when(lead)
    def _():
        extra[my, me, 3] = tile

    @pl.when(rest)
    def _():
        mine[3] = tile

    for n in range(3):
        for m in range(3):
            if n != m:
                high[n * rank : (n + 1) * rank, starts[m] : starts[m] + widths[m]] = jnp.zeros(
                    (rank, widths[m]), BF16
                )
    peak[...] = jnp.zeros_like(peak)
    for copy in fetch[3:6]:
        copy.wait()

    @pl.when(lead)
    def _():
        for copy in fetch_low(extra.at[my, me]):
            copy.wait()

    @pl.when(rest)
    def _():
        for copy in fetch_low(mine):
            copy.wait()

    @pl.when(rest)
    def _():
        give_own(me).start()

    @pl.when(rest & (first_core == 0))
    def _():
        pl.semaphore_wait(ready.at[1], 1)
        hop(1, 0, span(me, 0, half)).start()

    @pl.when(rest)
    def _():
        hand(2, 0, raw.at[partner]).wait_recv()
        for way in range(2):
            hop(way, 1, span(partner)).start()
        hop(1, 2, span(me, half, half)).start()

    @pl.when(lead)
    def _():
        give_own(partner).wait_recv()
        pass_on(0, 0, first_core).start()
        pl.semaphore_wait(ready.at[1], 1)
        pass_on(1, 0, first_core).start()
        slots = [(0, first_core)]
        for kk in range(hops):
            for way in ways(kk):
                chip = chip_of(way, kk)
                pass_on(way, kk, chip).wait_recv()
                if kk + 1 < hops and way in ways(kk + 1):
                    pass_on(way, kk + 1, chip).start()
                slots.append((slot_of(way, kk), chip))
        pl.semaphore_wait(barrier, models - 1)
        for slot, chip in slots:
            for copy in across(slot, chip):
                copy.start()
        for slot, chip in slots:
            for copy in across(slot, chip):
                copy.wait_recv()
            give(slot, chip).start()

    def unfold(slot, p, h):
        parts = [
            extra[quarter + h, p, n].astype(F32)
            for n in range(3)
            for quarter in range(0, models, 2)
        ]
        low_n[slot] = jnp.transpose(jnp.concatenate(parts, axis=0), (1, 0)).astype(BF16)

    def merge(p, first, rows, formed=False):
        at = pl.ds(pl.multiple_of(first, 16), rows)
        wide = 256
        for c in range(0, width, wide):
            cols = slice(c, c + wide)
            add = (
                whole[p, at, cols]
                if formed
                else jnp.dot(low_n[0], high[:, cols], preferred_element_type=F32)
            )
            new = raw[p, at, cols].astype(F32) + add
            whole[p, at, cols] = new
            peak[:, cols] = jnp.maximum(
                peak[:, cols], jnp.max(jnp.abs(new).reshape(rows // 8, 8, wide), axis=0)
            )

    def merge_some(number, which):
        @pl.loop(0, number)
        def _(n):
            p, h = which(n)
            unfold(0, p, h)
            merge(p, h * half, half)

    def given(slots):
        @pl.when(rest)
        def _():
            for slot in slots:
                give(slot, first_core).wait_recv()

    PARTS = (
        ((0, 1, 0, deep), (1, 1, 0, half)),
        ((1, 0, 0, deep),),
        ((0, 0, 0, deep), (1, 1, half, half)),
    )
    INDEX = (((0, 2, 0), (1, 3, 0)), ((1, 3, 1),), ((0, 2, 1), (1, 3, 2)))

    def merge_part(kk, part):
        chips = chip_of(0, kk), chip_of(1, kk)

        def way_chip(way):
            return chips[0] + way * (chips[1] - chips[0])

        if part == 0:
            given([slot_of(way, kk) for way in range(2)])
            merge_some(3, lambda n: (way_chip(lax.div(n, 2)) + 1, lax.rem(n, 2)))
        elif part == 1:
            merge_some(2, lambda n: (chips[1], n))
        else:
            merge_some(3, lambda n: (way_chip(lax.div(n, 2)) + lax.div(n, 2), lax.div(n + 1, 2)))

    def merge_own():
        given([0])

        @pl.when(lead)
        def _():
            hand(2, 0, raw.at[partner]).wait_recv()

        merge_some(4, lambda n: (first_core + lax.div(n, 2), lax.rem(n, 2)))

    far = chip_of(0, hops - 1)

    def far_products():
        given([slot_of(0, hops - 1)])

        @pl.loop(0, 4)
        def _(n):
            p, h = far + lax.div(n, 2), lax.rem(n, 2)
            unfold(0, p, h)
            at = pl.ds(pl.multiple_of(h * half, half), half)
            for c in range(0, width, 256):
                whole[p, at, c : c + 256] = jnp.dot(low_n[0], high[:, c : c + 256], preferred_element_type=F32)

    todo = [merge_own]
    events = [(kk, part) for kk in range(hops - 1) for part in range(3)]
    for e, (kk, part) in enumerate(events):
        last = kk == hops - 2

        @pl.when(rest)
        def _():
            for (way, piece, first, rows), (_, per_chip, place) in zip(PARTS[part], INDEX[part]):
                p, n = chip_of(way, kk) + piece, per_chip * kk + place
                hop(way, n, span(p, first, rows)).wait_recv()
                if not last:
                    hop(way, n + per_chip, span(p, first, rows)).start()
                elif piece != way:
                    for j, rows_j in enumerate(ROWS):
                        if way == 0 and j >= MOVED:

                            @pl.when(first_core != count - 2)
                            def _():
                                hop(way, LAST + j, span(p, *rows_j)).start()

                        else:
                            hop(way, LAST + j, span(p, *rows_j)).start()
                elif way == 1 and part == 2:

                    @pl.when(first_core == 2)
                    def _():
                        for j in range(MOVED, len(ROWS)):
                            moved(j, span(p, *ROWS[j])).start()

                hand(way, n, span(p, first, rows)).start()

        if e >= 2:
            todo.pop(0)()
        if e >= 4 and len(todo) > 1:
            todo.pop(0)()
        if e == len(events) - 2:
            far_products()

        @pl.when(lead)
        def _():
            for (way, piece, first, rows), (_, per_chip, place) in zip(PARTS[part], INDEX[part]):
                hand(way, per_chip * kk + place, span(chip_of(way, kk) + piece, first, rows)).wait_recv()

        todo.append(functools.partial(merge_part, kk, part))
    for task in todo:
        task()

    @pl.loop(0, count)
    def _(p):
        norms[:, p] = extra[:, p, 3]

    def sent(copies):
        for copy in copies:
            copy.wait_send()

    @pl.when(lead)
    def _():
        for slot in range(2 * hops):
            sent(across(slot, first_core) + [give(slot, first_core)])
        for kk in range(hops):
            sent([pass_on(way, kk, first_core) for way in ways(kk)])

    @pl.when(rest)
    def _():
        sent([give_own(me)])
        for kk, part in events:
            for (way, piece, first, rows), (_, per_chip, place) in zip(PARTS[part], INDEX[part]):
                n = per_chip * kk + place
                sent([hand(way, n, span(me, first, rows)), hop(way, n, span(me, first, rows))])

    sent([hand(2, 0, raw.at[me])])
    for j, (first, rows) in enumerate(ROWS):

        @pl.when(rest)
        def _():
            for way in range(2):
                hop(way, LAST + j, span(far + 1 - way, first, rows)).wait_recv()
                hand(way, LAST + j, span(far + 1 - way, first, rows)).start()

        @pl.when(lead)
        def _():
            for way in range(2):
                hand(way, LAST + j, span(far + 1 - way, first, rows)).wait_recv()

        for way in range(2):
            merge(far + 1 - way, first, rows, True)
    most[...] = peak[...]

    @pl.when(rest)
    def _():
        for way in range(2):
            for j, (first, rows) in enumerate(ROWS):
                sent([hand(way, LAST + j, span(me, first, rows))])
                if way == 1 or j < MOVED:
                    sent([hop(way, LAST + j, span(me, first, rows))])

    @pl.when(rest & (first_core != count - 2))
    def _():
        sent([hop(0, LAST + j, span(me, *ROWS[j])) for j in range(MOVED, len(ROWS))])

    @pl.when(rest & (first_core == 2))
    def _():
        sent([moved(j, span(me, *ROWS[j])) for j in range(MOVED, len(ROWS))])


def serve_kernel(
    whole, most, norms,
    q, k, v, scale_q, scale_k, scale_v, norm,
    q_out, k_out, v_out, scale_out, per, norm_f, norm_out,
    big_sem, sem,
):
    pieces, deep, width = whole.shape
    outs, stages = (q, k, v), (q_out, k_out, v_out)
    widths = tuple(a.shape[1] for a in outs)
    starts = (0, widths[0], widths[0] + widths[1])
    scale_out[...] = jnp.max(most[...], axis=0, keepdims=True)
    small = []
    for n, (dst, start, wide) in enumerate(zip((scale_q, scale_k, scale_v), starts, widths)):
        small.append(pltpu.make_async_copy(scale_out.at[:, pl.ds(start, wide)], dst, sem.at[n]))
    per[...] = 1.0 / scale_out[...]
    rows = 32

    ends = [sum(BLOCKS[:b]) for b in range(len(BLOCKS) + 1)]

    def out(n, b):
        at = pl.ds(ends[b] * deep, BLOCKS[b] * deep)
        return pltpu.make_async_copy(stages[n].at[at], outs[n].at[at], big_sem.at[n, b])

    for b in range(len(BLOCKS)):

        @pl.loop(ends[b], ends[b + 1])
        def _(p):
            @pl.loop(0, deep // rows)
            def _(r):
                here = pl.ds(pl.multiple_of(r * rows, rows), rows)
                there = pl.ds(pl.multiple_of(p * deep + r * rows, rows), rows)
                for n in range(3):
                    cols = slice(starts[n], starts[n] + widths[n])
                    stages[n][there, :] = (whole[p, here, cols] * per[:, cols]).astype(BF16)

        for n in range(3):
            out(n, b).start()

    models = norms.shape[0]
    wide = norm_f.shape[1] // 2
    for m in range(0, models, 2):
        pair = jnp.concatenate(
            [norms[n].astype(F32)[:, 0, :wide] for n in (m, m + 1)], axis=1
        )
        norm_f[pl.ds(m // 2, pieces, stride=models // 2), :] = pair
    norm_out[...] = norm_f[...].astype(BF16)
    small.append(pltpu.make_async_copy(norm_out, norm, sem.at[3]))
    for copy in small:
        copy.start()
    for copy in small:
        copy.wait()

    for b in range(len(BLOCKS)):
        for n in range(3):
            out(n, b).wait()


def local(count, models, q, low_q, high_q, k, low_k, high_k, v, low_v, high_v, norm_train, norm_step):
    deep, rank = low_q.shape
    widths = (q.shape[1], k.shape[1], v.shape[1])
    width = sum(widths)
    copies = 3 * (count // 4 - 1) + len(ROWS)
    piece = norm_train.shape[0]
    dma = pltpu.SemaphoreType.DMA
    anywhere = pl.BlockSpec(memory_space=pl.ANY)
    vmem = pl.BlockSpec(memory_space=pltpu.VMEM)
    whole, most, norms = pl.pallas_call(
        functools.partial(gather_kernel, count, models),
        out_shape=(
            pltpu.VMEM((count, deep, width), F32),
            pltpu.VMEM((8, width), F32),
            pltpu.VMEM((models, count, 8, 128), BF16),
        ),
        in_specs=[anywhere] * 11,
        out_specs=(vmem, vmem, vmem),
        scratch_shapes=[
            pltpu.VMEM((count, deep, width), BF16),
            pltpu.VMEM((models, count, 4, 8, 128), BF16),
            pltpu.VMEM((4, 8, 128), BF16),
            pltpu.VMEM((1, deep // 2, 3 * rank), BF16),
            pltpu.VMEM((3 * rank, width), BF16),
            pltpu.VMEM((2, 1, piece), F32),
            pltpu.VMEM((8, width), F32),
            dma((11,)),
            dma((count // 2, models - 1)),
            dma((count // 2, models - 1)),
            dma((2, count // 4)),
            dma((2, count // 4)),
            dma((count // 2 + 1,)),
            dma((count // 2 + 1,)),
            dma((2, copies + len(ROWS) - MOVED)),
            dma((2, copies)),
            dma((3, copies)),
            dma((3, copies)),
            pltpu.SemaphoreType.REGULAR((2,)),
        ],
        compiler_params=pltpu.CompilerParams(
            collective_id=0, has_side_effects=True, vmem_limit_bytes=20 * 2**20
        ),
        name="gather",
    )(
        *(
            pltpu.with_memory_space_constraint(a, pltpu.HBM)
            for a in (
                q, k, v, low_q.T, low_k.T, low_v.T, high_q, high_k, high_v,
                norm_train.reshape(1, piece), norm_step.reshape(1, piece),
            )
        )
    )
    total = count * deep
    sizes = tuple((total, w) for w in widths)
    serving_q, serving_k, serving_v, scale_q, scale_k, scale_v, norm = pl.pallas_call(
        serve_kernel,
        out_shape=tuple(jax.ShapeDtypeStruct(s, BF16) for s in sizes)
        + tuple(jax.ShapeDtypeStruct((1, w), F32) for w in widths)
        + (jax.ShapeDtypeStruct((count * models // 2, 2 * piece), BF16),),
        in_specs=[vmem] * 3,
        out_specs=(anywhere,) * 7,
        scratch_shapes=[pltpu.VMEM(s, BF16) for s in sizes]
        + [
            pltpu.VMEM((1, width), F32),
            pltpu.VMEM((1, width), F32),
            pltpu.VMEM((count * models // 2, 2 * piece), F32),
            pltpu.VMEM((count * models // 2, 2 * piece), BF16),
            dma((3, len(BLOCKS))),
            dma((4,)),
        ],
        compiler_params=pltpu.CompilerParams(vmem_limit_bytes=20 * 2**20),
        name="serve",
    )(*(pltpu.with_memory_space_constraint(a, pltpu.VMEM) for a in (whole, most, norms)))
    return (
        serving_q, serving_k, serving_v,
        scale_q.reshape(-1), scale_k.reshape(-1), scale_v.reshape(-1), norm.reshape(-1),
    )


def solution(mesh):
    in_specs = (
        P(("unit", "shard"), "model"),
        P(("unit", "shard"), None),
        P("unit", "model"),
        P(("unit", "shard"), "model"),
        P(("unit", "shard"), None),
        P("unit", "model"),
        P(("unit", "shard"), "model"),
        P(("unit", "shard"), None),
        P("unit", "model"),
        P(("unit", "shard", "model")),
        P(("unit", "shard", "model")),
    )
    out_specs = (
        P("unit", "model"),
        P("unit", "model"),
        P("unit", "model"),
        P(("unit", "model")),
        P(("unit", "model")),
        P(("unit", "model")),
        P("unit"),
    )
    body = functools.partial(local, mesh.shape["shard"], mesh.shape["model"])
    return jax.shard_map(body, mesh=mesh, in_specs=in_specs, out_specs=out_specs, check_vma=False)
```
